32 devices in a mesh: row: 4 (over y, core), col: 8 (over z, x).
Axes of the slice: x: 2, y: 2, z: 4, core: 2. Of those that a mesh axis runs over, the one named last changes fastest.
Arguments:
- vectors: bfloat16 [4, 8, 128, 384], P('row', 'col'), may hold values from -6 to 6
- near_blocks: bfloat16 [4, 8, 9, 384, 384], P('row', 'col'), may hold values from -0.15625 to 0.15625
- near_source: int32 [4, 8, 9], P('row', 'col'), may hold values from 0 to 8, each once within a row
- near_count: int32 [4, 8], P('row', 'col'), may hold values from 1 to 9
- basis_col: bfloat16 [4, 8, 64, 384], P('row', 'col'), may hold values from -0.3125 to 0.3125
- transfer_col: bfloat16 [4, 8, 64, 64], P('row', 'col'), may hold values from -0.25 to 0.25
- leaf_couple: bfloat16 [4, 8, 3, 5, 64, 64], P('row', 'col'), may hold values from -0.1875 to 0.1875
- coupling: bfloat16 [4, 4, 64, 64], P('row'), may hold values from -0.75 to 0.75
- distant_region_list: int32 [4, 4], P('row'), may hold values from 0 to 3, each once within a row
- transfer_row: bfloat16 [4, 8, 64, 64], P('row', 'col'), may hold values from -0.75 to 0.75
- basis_row: bfloat16 [4, 8, 64, 384], P('row', 'col'), may hold values from -0.75 to 0.75
Outputs:
- product: bfloat16 [4, 8, 128, 384], P('row', 'col')
The draws below stay inside these ranges and needn't reach their ends.
Inputs may be any that keep to these rules, and one draw needn't show every extreme that they name: `near_source`: the 9 slots of a leaf name the nine neighbourhood cells once each. Only the first near_count slots of a leaf are live. `distant_region_list`: each region's list names every region once.
All inputs are finite; a program needn't handle non-finite values.
Results may differ from the reference program's by a relative error of at most 0.013.
Values may be sent and summed in bfloat16 or wider, within the bound.
A program may use at most 64 MiB of HBM per device.

```python
import jax
import jax.numpy as jnp
from jax import lax

LEAF = 384
RANK = 64
NEAR = 9
VECS = 128
RFAR = 1
BAND = 5
N_ROW = 4
N_COL = 8


def touch_ends(array, key, least, high):
    place = [jax.random.randint(jax.random.fold_in(key, axis), (), 0, length) for axis, length in enumerate(array.shape)]
    main_axis = array.shape.index(max(array.shape))
    next_to = place[:main_axis] + [(place[main_axis] + 1) % array.shape[main_axis]] + place[main_axis + 1:]
    return array.at[tuple(place)].set(least).at[tuple(next_to)].set(high)


def steps_of(key, dims, shards, low, largest):
    level, own = 1.0, jax.random.fold_in(key, 6)
    for axis_at, shards_of in shards:
        heights = jnp.exp(jax.random.uniform(jax.random.fold_in(own, axis_at), (shards_of,), jnp.float32, low / len(shards), largest / len(shards)))
        level = level * jnp.repeat(heights, dims[axis_at] // shards_of).reshape([-1 if axis == axis_at else 1 for axis in range(len(dims))])
    return level


def normal_values(key, extent, width, limit, cuts=(), kind=jnp.bfloat16):
    values = width * jax.random.normal(key, extent, jnp.float32)
    if cuts:
        values = values * steps_of(key, extent, cuts, -0.22, 0.18)
    return jnp.clip(values, -limit, limit).astype(kind)


def setup_inputs(seed: int = 0) -> dict:
    splits = jax.random.split(jax.random.key(seed), 12)
    return {
        "vectors": normal_values(splits[0], (N_ROW, N_COL, VECS, LEAF), 1.0, 6.0, ((0, 4), (1, 8))),
        "near_blocks": normal_values(splits[1], (N_ROW, N_COL, NEAR, LEAF, LEAF), (LEAF * 4) ** -0.5, 0.15625, ((0, 4), (1, 8))),
        "near_source": jax.vmap(lambda own: jax.random.permutation(own, NEAR))(jax.random.split(splits[2], N_ROW * N_COL)).reshape((N_ROW, N_COL, NEAR)).astype(jnp.int32),
        "near_count": touch_ends(jax.random.randint(splits[3], (N_ROW, N_COL), 1, NEAR + 1), jax.random.fold_in(splits[3], 1), 1, NEAR).astype(jnp.int32),
        "basis_col": normal_values(splits[4], (N_ROW, N_COL, RANK, LEAF), LEAF ** -0.5, 0.3125, ((0, 4), (1, 8))),
        "transfer_col": normal_values(splits[5], (N_ROW, N_COL, RANK, RANK), (RANK * N_COL) ** -0.5, 0.25, ((0, 4), (1, 8))),
        "leaf_couple": normal_values(splits[6], (N_ROW, N_COL, 3, BAND, RANK, RANK), (RANK * 3 * BAND) ** -0.5, 0.1875, ((0, 4), (1, 8))),
        "coupling": normal_values(splits[7], (N_ROW, N_ROW, RANK, RANK), (RANK * RFAR) ** -0.5, 0.75, ((0, 4),)),
        "distant_region_list": jax.vmap(lambda own: jax.random.permutation(own, N_ROW))(jax.random.split(splits[8], N_ROW)).reshape((N_ROW, N_ROW)).astype(jnp.int32),
        "transfer_row": normal_values(splits[9], (N_ROW, N_COL, RANK, RANK), RANK ** -0.5, 0.75, ((0, 4), (1, 8))),
        "basis_row": normal_values(splits[10], (N_ROW, N_COL, RANK, LEAF), RANK ** -0.5, 0.75, ((0, 4), (1, 8))),
    }


def reference(vectors, near_blocks, near_source, near_count, basis_col, transfer_col, leaf_couple, coupling, distant_region_list, transfer_row, basis_row):
    upper_limit = lax.Precision.HIGHEST
    flat_vectors = vectors.reshape(N_ROW * N_COL, VECS, LEAF)
    row_identifiers = jnp.arange(N_ROW, dtype=jnp.int32)[:, None]
    col_ids = jnp.arange(N_COL, dtype=jnp.int32)[None, :]
    near = jnp.zeros((N_ROW, N_COL, VECS, LEAF), jnp.float32)
    for slot in range(NEAR):
        cell = near_source[:, :, slot]
        rows_src = (row_identifiers + cell // 3) % N_ROW
        cols_src = (col_ids + cell % 3) % N_COL
        flat = (rows_src * N_COL + cols_src).astype(jnp.int32)
        source = flat_vectors[flat].astype(jnp.float32)
        live = (near_count > slot).astype(jnp.float32)
        term = jnp.einsum("rcvp,rcpq->rcvq", source, near_blocks[:, :, slot].astype(jnp.float32), precision=upper_limit)
        near = near + live[:, :, None, None] * term
    incoming_leaf = jnp.einsum("rcvp,rckp->rcvk", vectors.astype(jnp.float32), basis_col.astype(jnp.float32), precision=upper_limit)
    band = jnp.zeros((N_ROW, N_COL, VECS, RANK), jnp.float32)
    for delta in range(3):
        for start_shift in range(BAND):
            shifted = jnp.roll(incoming_leaf, (-delta, -(3 + start_shift)), axis=(0, 1))
            band = band + jnp.einsum("rcvk,rckl->rcvl", shifted, leaf_couple[:, :, delta, start_shift].astype(jnp.float32), precision=upper_limit)
    incoming_region = jnp.einsum("rcvk,rckl->rvl", incoming_leaf, transfer_col.astype(jnp.float32), precision=upper_limit)
    region_ids = jnp.arange(N_ROW, dtype=jnp.int32)[:, None]
    far_mask = (((distant_region_list - region_ids) % N_ROW) >= 3).astype(jnp.float32)
    listed = incoming_region[distant_region_list] * far_mask[:, :, None, None]
    outgoing_region = jnp.einsum("ibne,iber->inr", listed, coupling.astype(jnp.float32), precision=upper_limit)
    leaf_out = band + jnp.einsum("rvk,rckl->rcvl", outgoing_region, transfer_row.astype(jnp.float32), precision=upper_limit)
    far = jnp.einsum("rcvk,rckq->rcvq", leaf_out, basis_row.astype(jnp.float32), precision=upper_limit)
    return (near + far).astype(jnp.bfloat16)
```

```python
import functools

import jax
import jax.numpy as jnp
from jax import lax
from jax.experimental import pallas as pl
from jax.experimental.pallas import tpu as pltpu
from jax.sharding import PartitionSpec as P

REACH = 3
MESH = pl.DeviceIdType.MESH
BF16 = jnp.bfloat16
F32 = jnp.float32


def dot(a, b, dims):
    return lax.dot_general(a, b, (dims, ((), ())), preferred_element_type=F32)


def kernel(
    rows,
    cols,
    source_hbm,
    count_hbm,
    list_hbm,
    vectors_hbm,
    blocks_hbm,
    basis_col_hbm,
    transfer_col_hbm,
    couple_hbm,
    coupling_hbm,
    transfer_row_hbm,
    basis_row_hbm,
    out_ref,
    source_ref,
    count_ref,
    list_ref,
    table,
    blocks,
    basis_col,
    transfer_col,
    couple,
    coupling,
    transfer_row,
    basis_row,
    leaf_send,
    up_send,
    reduced_send,
    leaf_buf,
    chunk_buf,
    region_buf,
    local_sems,
    near_send_sems,
    near_recv_sems,
    group_sems,
):
    r, c = lax.axis_index("row"), lax.axis_index("col")
    band = cols - REACH

    def behind(d, e):
        return (lax.rem(r + rows - d, rows), lax.rem(c + cols - e, cols))

    barrier = pltpu.get_barrier_semaphore()
    if rows * cols <= 64:
        for k in range(1, rows * cols):
            pl.semaphore_signal(barrier, inc=1, device_id=behind(k // cols, k % cols), device_id_type=MESH)
    else:

        @pl.loop(1, rows * cols)
        def _(k):
            pl.semaphore_signal(
                barrier, inc=1, device_id=behind(k // cols, lax.rem(k, cols)), device_id_type=MESH
            )

    loads = [
        pltpu.make_async_copy(src, dst, local_sems.at[i])
        for i, (src, dst) in enumerate(
            [
                (vectors_hbm, table.at[0]),
                (basis_col_hbm, basis_col),
                (transfer_col_hbm, transfer_col),
                (blocks_hbm, blocks),
                (couple_hbm, couple),
                (coupling_hbm, coupling),
                (transfer_row_hbm, transfer_row),
                (basis_row_hbm, basis_row),
                (source_hbm, source_ref),
                (count_hbm, count_ref),
                (list_hbm, list_ref),
            ]
        )
    ]
    for load in loads:
        load.start()
    for load in loads[:3]:
        load.wait()
    leaf_low = dot(basis_col[...], table[0], ((1,), (1,))).astype(BF16)
    leaf_send[...] = leaf_low
    up = dot(transfer_col[...], leaf_low, ((0,), (0,))).astype(BF16)
    chunk = up_send.shape[1]
    for e in range(cols):
        up_send[e] = up[e * chunk : (e + 1) * chunk]

    pl.semaphore_wait(barrier, rows * cols - 1)

    def remote(src, dst, send_sem, recv_sem, target):
        return pltpu.make_async_remote_copy(
            src_ref=src, dst_ref=dst, send_sem=send_sem, recv_sem=recv_sem,
            device_id=target, device_id_type=MESH,
        )

    parity = lax.rem(r, 2)
    partner = (r + 1 - 2 * parity, c)
    odd, even = parity == 1, parity == 0

    for e in range(1, cols):
        remote(
            up_send.at[lax.rem(c + cols - e, cols)], chunk_buf.at[e], group_sems.at[0], group_sems.at[1], behind(0, e)
        ).start()
    own_band = leaf_buf.at[pl.ds(0, band)]
    mid_band = leaf_buf.at[pl.ds(band, band)]
    top_band = leaf_buf.at[pl.ds(2 * band, band)]
    for j in range(band):
        remote(leaf_send, leaf_buf.at[j], group_sems.at[2], group_sems.at[3], behind(0, REACH + j)).start()
    near = {}
    for d, e in ((2, 0), (0, 2), (0, 1), (2, 1), (2, 2)):
        cell = d * REACH + e
        near[cell] = remote(
            table.at[0], table.at[cell], near_send_sems.at[cell], near_recv_sems.at[cell], behind(d, e)
        )
        near[cell].start()
    for e in range(REACH):
        cell = REACH + e
        near[cell] = remote(
            table.at[2 * REACH * (1 - parity) + e],
            table.at[cell],
            near_send_sems.at[cell],
            near_recv_sems.at[cell],
            partner,
        )
    band_up = remote(own_band, top_band, group_sems.at[4], group_sems.at[5], behind(2, 0))
    band_across = remote(
        leaf_buf.at[pl.ds(2 * band * (1 - parity), band)], mid_band, group_sems.at[6], group_sems.at[7], partner
    )

    def start_if(condition, copy):
        @pl.when(condition)
        def _():
            copy.start()

    start_if(odd, near[REACH])
    for load in loads[3:]:
        load.wait()

    count = count_ref[0, 0]

    def term(cell):
        slot = jnp.int32(0)
        for s in range(source_ref.shape[0]):
            slot = jnp.where(source_ref[s] == cell, s, slot)
        source = table[cell]
        source = jnp.where(slot < count, source, jnp.zeros_like(source))
        return dot(source, blocks[slot], ((1,), (0,)))

    arrived = chunk_buf.at[pl.ds(1, cols - 1)]
    pltpu.make_async_copy(arrived, arrived, group_sems.at[1]).wait()
    reduced = up_send[c].astype(F32)
    for e in range(1, cols):
        reduced = reduced + chunk_buf[e].astype(F32)
    reduced_send[...] = reduced.astype(BF16)
    pltpu.make_async_copy(own_band, own_band, group_sems.at[3]).wait()
    band_up.start()
    start_if(odd, band_across)
    total = term(0)
    for d in range(REACH, rows):
        for e in range(cols):
            remote(
                reduced_send, region_buf.at[d - REACH, c], group_sems.at[8], group_sems.at[9], behind(d, e)
            ).start()

    near[2 * REACH].wait_recv()
    start_if(even, near[REACH])
    total = total + term(2 * REACH)
    band_up.wait_recv()
    start_if(even, band_across)
    for e in (2, 1):
        near[e].wait_recv()
        start_if(odd, near[REACH + e])
        total = total + term(e)
    near[REACH].wait_recv()
    total = total + term(REACH)

    pltpu.make_async_copy(region_buf, region_buf, group_sems.at[9]).wait()
    rank, vecs = leaf_buf.shape[1:]
    region_out = None
    for d in range(REACH, rows):
        target = lax.rem(r + d, rows)
        slot = jnp.int32(0)
        for f in range(rows):
            slot = jnp.where(list_ref[f] == target, f, slot)
        region = region_buf[d - REACH].astype(F32).reshape(rank, vecs).astype(BF16)
        part = dot(coupling[slot], region, ((0,), (0,)))
        region_out = part if region_out is None else region_out + part
    leaf_out = dot(transfer_row[...], region_out.astype(BF16), ((0,), (0,)))
    band_across.wait_recv()
    leaf_out = leaf_out + dot(
        couple[...].reshape(REACH * band * rank, rank),
        leaf_buf[...].reshape(REACH * band * rank, vecs),
        ((0,), (0,)),
    )
    total = total + dot(leaf_out.astype(BF16), basis_row[...], ((0,), (0,)))

    for e in (1, 2):
        near[2 * REACH + e].wait_recv()
        start_if(even, near[REACH + e])
        total = total + term(2 * REACH + e)
    for e in (1, 2):
        near[REACH + e].wait_recv()
        total = total + term(REACH + e)
    out_ref[...] = total.astype(out_ref.dtype)

    for copy in near.values():
        copy.wait_send()
    band_up.wait_send()
    band_across.wait_send()
    pltpu.make_async_copy(arrived, arrived, group_sems.at[0]).wait()
    pltpu.make_async_copy(own_band, own_band, group_sems.at[2]).wait()
    pltpu.make_async_copy(region_buf, region_buf, group_sems.at[8]).wait()


def per_device(
    vectors,
    near_blocks,
    near_source,
    near_count,
    basis_col,
    transfer_col,
    leaf_couple,
    coupling,
    distant_region_list,
    transfer_row,
    basis_row,
):
    rows, cols = lax.axis_size("row"), lax.axis_size("col")
    vecs, leaf = vectors.shape[2:]
    rank = basis_col.shape[2]
    cells = near_blocks.shape[2]
    band = leaf_couple.shape[3]
    hbm = pl.BlockSpec(memory_space=pl.ANY)
    out = pl.pallas_call(
        functools.partial(kernel, rows, cols),
        out_shape=pltpu.VMEM((vecs, leaf), BF16),
        in_specs=[hbm] * 11,
        out_specs=pl.BlockSpec(memory_space=pltpu.VMEM),
        scratch_shapes=[
            pltpu.SMEM((cells,), jnp.int32),
            pltpu.SMEM((1, 1), jnp.int32),
            pltpu.SMEM((rows,), jnp.int32),
            pltpu.VMEM((cells, vecs, leaf), BF16),
            pltpu.VMEM((cells, leaf, leaf), BF16),
            pltpu.VMEM((rank, leaf), BF16),
            pltpu.VMEM((rank, rank), BF16),
            pltpu.VMEM((REACH * band, rank, rank), BF16),
            pltpu.VMEM((rows, rank, rank), BF16),
            pltpu.VMEM((rank, rank), BF16),
            pltpu.VMEM((rank, leaf), BF16),
            pltpu.VMEM((rank, vecs), BF16),
            pltpu.VMEM((cols, rank // cols, vecs), BF16),
            pltpu.VMEM((rank // cols, vecs), BF16),
            pltpu.VMEM((REACH * band, rank, vecs), BF16),
            pltpu.VMEM((cols, rank // cols, vecs), BF16),
            pltpu.VMEM((rows - REACH, cols, rank // cols, vecs), BF16),
            pltpu.SemaphoreType.DMA((11,)),
            pltpu.SemaphoreType.DMA((cells,)),
            pltpu.SemaphoreType.DMA((cells,)),
            pltpu.SemaphoreType.DMA((10,)),
        ],
        compiler_params=pltpu.CompilerParams(collective_id=0, has_side_effects=True),
    )(
        near_source[0, 0],
        near_count,
        distant_region_list[0],
        vectors[0, 0],
        near_blocks[0, 0],
        basis_col[0, 0],
        transfer_col[0, 0],
        leaf_couple[0, 0].reshape(REACH * band, rank, rank),
        coupling[0],
        transfer_row[0, 0],
        basis_row[0, 0],
    )
    return out[None, None]


def solution(mesh):
    placed = (
        P("row", "col", None, None),
        P("row", "col", None, None, None),
        P("row", "col", None),
        P("row", "col"),
        P("row", "col", None, None),
        P("row", "col", None, None),
        P("row", "col", None, None, None, None),
        P("row", None, None, None),
        P("row", None),
        P("row", "col", None, None),
        P("row", "col", None, None),
    )
    return jax.shard_map(
        per_device,
        mesh=mesh,
        in_specs=placed,
        out_specs=P("row", "col", None, None),
        check_vma=False,
    )
```

```python
import functools

import jax
import jax.numpy as jnp
from jax import lax
from jax.experimental import pallas as pl
from jax.experimental.pallas import tpu as pltpu
from jax.sharding import PartitionSpec as P

REACH = 3
PIECES = 2
MESH = pl.DeviceIdType.MESH
BF16 = jnp.bfloat16
F32 = jnp.float32


def dot(a, b, dims):
    return lax.dot_general(a, b, (dims, ((), ())), preferred_element_type=F32)


def kernel(
    rows,
    cols,
    source_hbm,
    count_hbm,
    list_hbm,
    vectors_hbm,
    blocks_hbm,
    basis_col_hbm,
    transfer_col_hbm,
    couple_hbm,
    coupling_hbm,
    transfer_row_hbm,
    basis_row_hbm,
    out_ref,
    source_ref,
    count_ref,
    list_ref,
    table,
    blocks,
    basis_col,
    transfer_col,
    couple,
    coupling,
    transfer_row,
    basis_row,
    leaf_send,
    up_send,
    reduced_send,
    leaf_buf,
    chunk_buf,
    region_buf,
    local_sems,
    near_send_sems,
    near_recv_sems,
    own_sems,
    up_send_sems,
    up_recv_sems,
    across_send_sems,
    across_recv_sems,
    group_sems,
    near_sem,
    far_sem,
):
    r, c = lax.axis_index("row"), lax.axis_index("col")
    parity = lax.rem(r, 2)
    band = cols - REACH
    near_reach = REACH - 1
    n_red, chunk = up_send.shape[0], up_send.shape[1]
    first_red = (cols - n_red) // 2
    is_red = jnp.logical_and(c >= first_red, c < first_red + n_red)

    def behind(d, e):
        return (lax.rem(r + rows - d, rows), lax.rem(c + cols - e, cols))

    def when(condition, act):
        @pl.when(condition)
        def _():
            act()

    loads = [
        pltpu.make_async_copy(src, dst, local_sems.at[i])
        for i, (src, dst) in enumerate(
            [
                (vectors_hbm, table.at[0]),
                (basis_col_hbm, basis_col),
                (transfer_col_hbm, transfer_col),
                (blocks_hbm, blocks),
                (couple_hbm, couple),
                (coupling_hbm, coupling),
                (transfer_row_hbm, transfer_row),
                (basis_row_hbm, basis_row),
                (source_hbm, source_ref),
                (count_hbm, count_ref),
                (list_hbm, list_ref),
            ]
        )
    ]
    for load in loads[:3]:
        load.start()

    barrier = pltpu.get_barrier_semaphore()

    def greet(sem, e, row_from=0, row_to=rows, row_not=rows):
        def one(row):
            pl.semaphore_signal(sem, inc=1, device_id=(row, lax.rem(c + cols - e, cols)), device_id_type=MESH)

        if rows <= 4:
            for row in range(rows):
                if isinstance(row_from, int) and isinstance(row_to, int):
                    one(row)
                else:
                    wanted = jnp.logical_and(row >= row_from, row < row_to)
                    when(jnp.logical_and(wanted, row != row_not), functools.partial(one, row))
        else:

            @pl.loop(row_from, row_to)
            def _(row):
                when(row != row_not, functools.partial(one, row))

    def greet_columns(low, high, condition, sem):
        if cols <= 8:
            for e in range(low, high):
                when(condition(e), functools.partial(greet, sem, e))
        else:

            @pl.loop(low, high)
            def _(e):
                when(condition(e), functools.partial(greet, sem, e))

    greet(barrier, 0, r + 1 - parity * 2, rows, r)
    greet_columns(1, cols, lambda e: c < e, barrier)

    for load in loads[3:]:
        load.start()
    for load in loads[:3]:
        load.wait()
    leaf_low = dot(basis_col[...], table[0], ((1,), (1,))).astype(BF16)
    leaf_send[...] = leaf_low
    up = dot(transfer_col[...], leaf_low, ((0,), (0,))).astype(BF16)
    for j in range(n_red):
        up_send[j] = up[j * chunk : (j + 1) * chunk]

    def remote(src, dst, send_sem, recv_sem, target):
        return pltpu.make_async_remote_copy(
            src_ref=src, dst_ref=dst, send_sem=send_sem, recv_sem=recv_sem,
            device_id=target, device_id_type=MESH,
        )

    side = lax.rem(c, 2)
    passes, direct = side == 0, side == 1
    partner = (r + 1 - 2 * parity, c)
    odd, even = parity == 1, parity == 0
    group = -(-band // up_send_sems.shape[0])
    spans = [(j, min(group, band - j)) for j in range(0, band, group)]

    pieces = near_send_sems.shape[1]
    part = table.shape[1] // pieces

    def near_copies(source, cell, target):
        return [
            remote(
                table.at[source, pl.ds(p * part, part)], table.at[cell, pl.ds(p * part, part)],
                near_send_sems.at[cell, p], near_recv_sems.at[cell, p], target,
            )
            for p in range(pieces)
        ]

    near = {}
    for d, e in ((2, 0), (0, 2), (2, 2)):
        near[d * REACH + e] = near_copies(0, d * REACH + e, behind(d, e))
    for d in (0, 2):
        cell = d * REACH + 1
        row, col = behind(d, 1)
        near[cell] = near_copies(
            (cell + 1) * (1 - side), cell, (jnp.where(passes, r, row), jnp.where(passes, c + 1, col))
        )
    for e in range(REACH):
        near[REACH + e] = near_copies(2 * REACH * (1 - parity) + e, REACH + e, partner)
    chunks = [
        remote(
            up_send.at[j],
            chunk_buf.at[lax.rem(c + cols - (first_red + j), cols)],
            group_sems.at[0],
            group_sems.at[1],
            (r, first_red + j),
        )
        for j in range(n_red)
    ]
    leaves = [
        remote(leaf_send, leaf_buf.at[j], group_sems.at[2], own_sems.at[j // group], behind(0, REACH + j))
        for j in range(band)
    ]
    band_up = [
        remote(
            leaf_buf.at[pl.ds(j, n)], leaf_buf.at[pl.ds(2 * band + j, n)],
            up_send_sems.at[j // group], up_recv_sems.at[j // group], behind(2, 0),
        )
        for j, n in spans
    ]
    band_across = [
        remote(
            leaf_buf.at[pl.ds(2 * band * (1 - parity) + j, n)], leaf_buf.at[pl.ds(band + j, n)],
            across_send_sems.at[j // group], across_recv_sems.at[j // group], partner,
        )
        for j, n in spans
    ]

    def sends(stage):
        def column(e):
            return c >= e if stage == 0 else c < e

        for j in range(n_red):
            up_by = first_red + j - c
            if stage == 0:
                known = up_by < 0
            elif stage == 1:
                known = jnp.logical_and(up_by > 0, up_by <= near_reach)
            else:
                known = up_by > near_reach
            when(known, chunks[j].start)
        for j in range(band):
            e = REACH + j
            if stage != (1 if cols - e > near_reach else 2):
                when(column(e), leaves[j].start)
        if stage != 1:
            for d in (0, 2):
                for near_copy in near[d * REACH + 2]:
                    when(column(2), near_copy.start)
        if stage == 0:
            for d in (0, 2):
                for near_copy in near[d * REACH + 1]:
                    when(direct, near_copy.start)
        if stage != 2:
            below = r >= 2
            for near_copy in near[2 * REACH]:
                when(below if stage == 0 else jnp.logical_not(below), near_copy.start)

    higher = cols - 1 - c
    close = jnp.minimum(near_reach, higher)
    pl.semaphore_wait(barrier, r + rows * c + 1 - parity)
    greet(near_sem, 0, 0, r - parity)
    greet_columns(1, near_reach + 1, lambda e: c >= e, near_sem)
    greet_columns(near_reach + 1, cols, lambda e: c >= e, far_sem)
    sends(0)
    above = rows - 2 - r + parity + rows * close
    when(above > 0, lambda: pl.semaphore_wait(near_sem, above))
    sends(1)

    for near_copy in near[REACH]:
        when(odd, near_copy.start)
    for load in loads[3:]:
        load.wait()

    count = count_ref[0, 0]

    def term(cell):
        slot = jnp.int32(0)
        for s in range(source_ref.shape[0]):
            slot = jnp.where(source_ref[s] == cell, s, slot)
        source = table[cell]
        source = jnp.where(slot < count, source, jnp.zeros_like(source))
        return dot(source, blocks[slot], ((1,), (0,)))

    total = term(0)
    distant = rows * (higher - close)
    when(distant > 0, lambda: pl.semaphore_wait(far_sem, distant))
    sends(2)

    arrived = chunk_buf.at[pl.ds(1, cols - 1)]

    @pl.when(is_red)
    def _():
        pltpu.make_async_copy(arrived, arrived, group_sems.at[1]).wait()
        reduced = up_send[jnp.clip(c - first_red, 0, n_red - 1)].astype(F32)
        for e in range(1, cols):
            reduced = reduced + chunk_buf[e].astype(F32)
        reduced_send[...] = reduced.astype(BF16)
        for d in range(REACH, rows):
            for e in range(cols):
                remote(
                    reduced_send, region_buf.at[d - REACH, c - first_red], group_sems.at[4], group_sems.at[5],
                    behind(d, e),
                ).start()

    def got(d, e):
        cell = d * REACH + e
        for p in range(pieces):
            near[cell][p].wait_recv()
            if (d, e) != (0, 0):
                when(odd if d == 0 else even, near[REACH + e][p].start)
            if e == 2:
                when(passes, near[cell - 1][p].start)

    def own_groups(lo, hi):
        for g in range(lo, hi):
            j, n = spans[g]
            view = leaf_buf.at[pl.ds(j, n)]
            pltpu.make_async_copy(view, view, own_sems.at[g]).wait()
            band_up[g].start()
            when(odd, band_across[g].start)

    def here(cell):
        for near_copy in near[cell]:
            near_copy.wait_recv()
        return term(cell)

    own_groups(0, len(spans))
    got(0, 2)
    got(2, 2)
    got(2, 0)
    for g in range(len(spans)):
        band_up[g].wait_recv()
        when(even, band_across[g].start)
    for cell in (2 * REACH, 2, 2 * REACH + 2):
        total = total + term(cell)
    total = total + here(REACH)
    got(0, 1)
    total = total + term(1)

    pltpu.make_async_copy(region_buf, region_buf, group_sems.at[5]).wait()
    rank, vecs = leaf_buf.shape[1:]
    region_out = None
    for d in range(REACH, rows):
        target = lax.rem(r + d, rows)
        slot = jnp.int32(0)
        for f in range(rows):
            slot = jnp.where(list_ref[f] == target, f, slot)
        region = region_buf[d - REACH].astype(F32).reshape(rank, vecs).astype(BF16)
        product = dot(coupling[slot], region, ((0,), (0,)))
        region_out = product if region_out is None else region_out + product
    leaf_out = dot(transfer_row[...], region_out.astype(BF16), ((0,), (0,)))
    for g in range(len(spans)):
        band_across[g].wait_recv()
    leaf_out = leaf_out + dot(
        couple[...].reshape(REACH * band * rank, rank),
        leaf_buf[...].reshape(REACH * band * rank, vecs),
        ((0,), (0,)),
    )
    total = total + dot(leaf_out.astype(BF16), basis_row[...], ((0,), (0,)))
    got(2, 1)
    total = total + term(2 * REACH + 1)
    total = total + here(REACH + 2)
    total = total + here(REACH + 1)
    out_ref[...] = total.astype(out_ref.dtype)

    for copies in near.values():
        for copy in copies:
            copy.wait_send()
    for copy in band_up + band_across:
        copy.wait_send()

    own_band = leaf_buf.at[pl.ds(0, band)]
    pltpu.make_async_copy(own_band, own_band, group_sems.at[2]).wait()

    @pl.when(is_red)
    def _():
        others = up_send.at[pl.ds(1, n_red - 1)]
        pltpu.make_async_copy(others, others, group_sems.at[0]).wait()
        for d in range(REACH, rows):
            pltpu.make_async_copy(chunk_buf, chunk_buf, group_sems.at[4]).wait()

    @pl.when(jnp.logical_not(is_red))
    def _():
        pltpu.make_async_copy(up_send, up_send, group_sems.at[0]).wait()


def per_device(
    vectors,
    near_blocks,
    near_source,
    near_count,
    basis_col,
    transfer_col,
    leaf_couple,
    coupling,
    distant_region_list,
    transfer_row,
    basis_row,
):
    rows, cols = lax.axis_size("row"), lax.axis_size("col")
    vecs, leaf = vectors.shape[2:]
    rank = basis_col.shape[2]
    cells = near_blocks.shape[2]
    band = leaf_couple.shape[3]
    n_red = cols // 2
    groups = min(band, 5)
    groups = -(-band // -(-band // groups))
    hbm = pl.BlockSpec(memory_space=pl.ANY)
    out = pl.pallas_call(
        functools.partial(kernel, rows, cols),
        out_shape=pltpu.VMEM((vecs, leaf), BF16),
        in_specs=[hbm] * 11,
        out_specs=pl.BlockSpec(memory_space=pltpu.VMEM),
        scratch_shapes=[
            pltpu.SMEM((cells,), jnp.int32),
            pltpu.SMEM((1, 1), jnp.int32),
            pltpu.SMEM((rows,), jnp.int32),
            pltpu.VMEM((cells, vecs, leaf), BF16),
            pltpu.VMEM((cells, leaf, leaf), BF16),
            pltpu.VMEM((rank, leaf), BF16),
            pltpu.VMEM((rank, rank), BF16),
            pltpu.VMEM((REACH * band, rank, rank), BF16),
            pltpu.VMEM((rows, rank, rank), BF16),
            pltpu.VMEM((rank, rank), BF16),
            pltpu.VMEM((rank, leaf), BF16),
            pltpu.VMEM((rank, vecs), BF16),
            pltpu.VMEM((n_red, rank // n_red, vecs), BF16),
            pltpu.VMEM((rank // n_red, vecs), BF16),
            pltpu.VMEM((REACH * band, rank, vecs), BF16),
            pltpu.VMEM((cols, rank // n_red, vecs), BF16),
            pltpu.VMEM((rows - REACH, n_red, rank // n_red, vecs), BF16),
            pltpu.SemaphoreType.DMA((11,)),
            pltpu.SemaphoreType.DMA((cells, PIECES)),
            pltpu.SemaphoreType.DMA((cells, PIECES)),
            pltpu.SemaphoreType.DMA((groups,)),
            pltpu.SemaphoreType.DMA((groups,)),
            pltpu.SemaphoreType.DMA((groups,)),
            pltpu.SemaphoreType.DMA((groups,)),
            pltpu.SemaphoreType.DMA((groups,)),
            pltpu.SemaphoreType.DMA((6,)),
            pltpu.SemaphoreType.REGULAR,
            pltpu.SemaphoreType.REGULAR,
        ],
        compiler_params=pltpu.CompilerParams(collective_id=0, has_side_effects=True),
    )(
        near_source[0, 0],
        near_count,
        distant_region_list[0],
        vectors[0, 0],
        near_blocks[0, 0],
        basis_col[0, 0],
        transfer_col[0, 0],
        leaf_couple[0, 0].reshape(REACH * band, rank, rank),
        coupling[0],
        transfer_row[0, 0],
        basis_row[0, 0],
    )
    return out[None, None]


def solution(mesh):
    placed = (
        P("row", "col", None, None),
        P("row", "col", None, None, None),
        P("row", "col", None),
        P("row", "col"),
        P("row", "col", None, None),
        P("row", "col", None, None),
        P("row", "col", None, None, None, None),
        P("row", None, None, None),
        P("row", None),
        P("row", "col", None, None),
        P("row", "col", None, None),
    )
    return jax.shard_map(
        per_device,
        mesh=mesh,
        in_specs=placed,
        out_specs=P("row", "col", None, None),
        check_vma=False,
    )
```

```python
import functools

import jax
import jax.numpy as jnp
from jax import lax
from jax.experimental import pallas as pl
from jax.experimental.pallas import tpu as pltpu
from jax.sharding import PartitionSpec as P

REACH = 3
PIECES = 4
MESH = pl.DeviceIdType.MESH
BF16 = jnp.bfloat16
F32 = jnp.float32


def dot(a, b, dims):
    return lax.dot_general(a, b, (dims, ((), ())), preferred_element_type=F32)


def kernel(
    rows,
    cols,
    source_hbm,
    count_hbm,
    list_hbm,
    vectors_hbm,
    blocks_hbm,
    basis_col_hbm,
    transfer_col_hbm,
    couple_hbm,
    coupling_hbm,
    transfer_row_hbm,
    basis_row_hbm,
    out_ref,
    source_ref,
    count_ref,
    list_ref,
    table,
    blocks,
    basis_col,
    transfer_col,
    couple,
    coupling,
    transfer_row,
    basis_row,
    leaf_send,
    up_send,
    reduced_send,
    leaf_buf,
    chunk_buf,
    region_buf,
    local_sems,
    near_recv_sems,
    own_sems,
    up_recv_sems,
    group_sems,
    near_sem,
    far_sem,
    region_sem,
):
    r, c = lax.axis_index("row"), lax.axis_index("col")
    parity = lax.rem(r, 2)
    band = cols - REACH
    near_reach = REACH - 1
    n_red, chunk = up_send.shape[0], up_send.shape[1]
    first_red = n_red
    is_red = jnp.logical_and(c >= first_red, c < first_red + n_red)

    def behind(d, e):
        return (lax.rem(r + rows - d, rows), lax.rem(c + cols - e, cols))

    def when(condition, act):
        @pl.when(condition)
        def _():
            act()

    loads = [
        pltpu.make_async_copy(src, dst, local_sems.at[i])
        for i, (src, dst) in enumerate(
            [
                (vectors_hbm, table.at[0]),
                (basis_col_hbm, basis_col),
                (transfer_col_hbm, transfer_col),
                (blocks_hbm, blocks),
                (couple_hbm, couple),
                (coupling_hbm, coupling),
                (transfer_row_hbm, transfer_row),
                (basis_row_hbm, basis_row),
                (source_hbm, source_ref),
                (count_hbm, count_ref),
                (list_hbm, list_ref),
            ]
        )
    ]
    for load in loads[:3]:
        load.start()

    barrier = pltpu.get_barrier_semaphore()

    def place(row, col):
        return ((row // 2 + col // 2 + lax.rem(col, 2)) * cols + col) * rows + row

    mine = place(r, c)

    def near_column(col):
        return jnp.abs(col - c) <= near_reach

    far_rows = rows - REACH
    one = jnp.bool_(True)

    def to_row(k):
        return one, behind(0, k + 1)

    def to_facing(k):
        return one, behind(rows - 2 + 4 * k if rows > 4 else 2, 0)

    def to_targets(k):
        return is_red, behind(REACH + k // cols, k % cols)

    def to_reducers(k):
        return one, (lax.rem(r + REACH + k // n_red, rows), first_red + k % n_red)

    kinds = [
        (cols - 1, to_row, near_column),
        (2 if rows > 4 else 1, to_facing, lambda col: one),
        (far_rows * cols, to_targets, None),
        (far_rows * n_red, to_reducers, None),
    ]

    def greet(sem, device):
        pl.semaphore_signal(sem, inc=1, device_id=device, device_id_type=MESH)

    def greet_all(down):
        for number, which, is_near in kinds:

            def act(k, which=which, is_near=is_near):
                valid, device = which(k)
                if not down:
                    when(jnp.logical_and(valid, place(*device) > mine), functools.partial(greet, barrier, device))
                    return
                below = jnp.logical_and(valid, place(*device) < mine)
                if is_near is None:
                    if which is to_reducers:
                        when(below, functools.partial(greet, region_sem, device))
                    return
                close = is_near(device[1])
                when(jnp.logical_and(below, close), functools.partial(greet, near_sem, device))
                when(jnp.logical_and(below, jnp.logical_not(close)), functools.partial(greet, far_sem, device))

            if number <= 16:
                for k in range(number):
                    act(k)
            else:
                pl.loop(0, number)(act)

    def count_all(numbers):
        for number, which, is_near in kinds:

            def add(k, numbers, which=which, is_near=is_near):
                valid, device = which(k)
                above = place(*device) > mine
                no = jnp.logical_not(one)
                if is_near is None:
                    found = (jnp.logical_not(above), no, no, above if which is to_targets else no)
                else:
                    close = is_near(device[1])
                    found = (
                        jnp.logical_not(above),
                        jnp.logical_and(above, close),
                        jnp.logical_and(above, jnp.logical_not(close)),
                        no,
                    )
                return tuple(n + jnp.where(jnp.logical_and(valid, f), 1, 0) for n, f in zip(numbers, found))

            if number <= 16:
                for k in range(number):
                    numbers = add(k, numbers)
            else:
                numbers = lax.fori_loop(0, number, add, numbers)
        return numbers

    greet(barrier, (r + 1 - 2 * parity, c))
    greet_all(False)
    zero = jnp.int32(0)
    n_below, n_near_above, n_far_above, n_region_above = count_all((jnp.int32(1), zero, zero, zero))

    for load in loads[3:]:
        load.start()
    pl.semaphore_wait(barrier, n_below)
    greet_all(True)
    for load in loads[:3]:
        load.wait()
    leaf_low = dot(basis_col[...], table[0], ((1,), (1,))).astype(BF16)
    leaf_send[...] = leaf_low
    up = dot(transfer_col[...], leaf_low, ((0,), (0,))).astype(BF16)
    for j in range(n_red):
        up_send[j] = up[j * chunk : (j + 1) * chunk]

    def remote(src, dst, send_sem, recv_sem, target):
        return pltpu.make_async_remote_copy(
            src_ref=src, dst_ref=dst, send_sem=send_sem, recv_sem=recv_sem,
            device_id=target, device_id_type=MESH,
        )

    side = lax.rem(c, 2)
    passes, direct = side == 0, side == 1
    partner = (r + 1 - 2 * parity, c)
    odd, even = parity == 1, parity == 0
    group = -(-band // own_sems.shape[0])
    spans = [(j, min(group, band - j)) for j in range(0, band, group)]

    pieces = near_recv_sems.shape[1]
    part = table.shape[1] // pieces

    def near_copies(source, cell, target):
        return [
            remote(
                table.at[source, pl.ds(p * part, part)], table.at[cell, pl.ds(p * part, part)],
                group_sems.at[2], near_recv_sems.at[cell - 1, p], target,
            )
            for p in range(pieces)
        ]

    beside = (r, c + 1 - 2 * side)
    near = {
        2 * REACH: near_copies(0, 2 * REACH, behind(2, 0)),
        2: near_copies(0, 2, behind(0, 2)),
        2 * REACH + 2: near_copies(2 * REACH, 2 * REACH + 2, behind(0, 2)),
    }
    last, end = c >= cols - near_reach, c == cols - 1
    around = {e: near_copies(e, 2 * REACH + e, behind(2, 0)) for e in (1, 2)}
    first_to_end = near_copies(0, 1, (r, cols - 1))
    for d in (0, 2):
        near[d * REACH + 1] = near_copies(d * REACH + 2 * (1 - side), d * REACH + 1, beside)
    for e in range(REACH):
        near[REACH + e] = near_copies(2 * REACH * (1 - parity) + e, REACH + e, partner)

    chunks = [
        remote(
            up_send.at[j],
            chunk_buf.at[lax.rem(c + cols - (first_red + j), cols)],
            group_sems.at[0],
            group_sems.at[1],
            (r, first_red + j),
        )
        for j in range(n_red)
    ]
    leaves = [
        remote(leaf_send, leaf_buf.at[j], group_sems.at[3], own_sems.at[j // group], behind(0, REACH + j))
        for j in range(band)
    ]
    band_up = [
        remote(
            leaf_buf.at[pl.ds(j, n)], leaf_buf.at[pl.ds(2 * band + j, n)],
            group_sems.at[3], up_recv_sems.at[j // group], behind(2, 0),
        )
        for j, n in spans
    ]
    band_across = [
        remote(
            leaf_buf.at[pl.ds(2 * band * (1 - parity) + j, n)], leaf_buf.at[pl.ds(band + j, n)],
            group_sems.at[3], group_sems.at[6], partner,
        )
        for j, n in spans
    ]

    def known(target, stage, is_near=None):
        below = place(*target) < mine
        if stage == 0:
            return below
        close = near_column(target[1])
        return jnp.logical_and(jnp.logical_not(below), close if stage == 1 else jnp.logical_not(close))

    def start_all(copies, condition):
        for copy in copies:
            when(condition, copy.start)

    def sends(stage):
        if stage != 2:
            start_all(near[2 * REACH], known(behind(2, 0), stage))
        for j in range(n_red):
            target = (r, first_red + j)
            when(jnp.logical_and(known(target, stage), target[1] != c), chunks[j].start)
        for j in range(band):
            when(known(behind(0, REACH + j), stage), leaves[j].start)
        if stage != 2:
            start_all(near[2], known(behind(0, 2), stage))
        if stage == 0:
            start_all(near[1], direct)

    sends(0)
    when(n_near_above > 0, lambda: pl.semaphore_wait(near_sem, n_near_above))
    sends(1)

    for near_copy in near[REACH]:
        when(odd, near_copy.start)
    for load in loads[3:]:
        load.wait()

    count = count_ref[0, 0]

    def term(cell):
        slot = jnp.int32(0)
        for s in range(source_ref.shape[0]):
            slot = jnp.where(source_ref[s] == cell, s, slot)
        source = table[cell]
        source = jnp.where(slot < count, source, jnp.zeros_like(source))
        return dot(source, blocks[slot], ((1,), (0,)))

    total = term(0)
    wraps = known(behind(0, 2), 2)

    def facing_arrived(pass_on):
        for p in range(pieces):
            near[2 * REACH][p].wait_recv()
            if pass_on:
                near[2 * REACH + 2][p].start()
            when(direct, near[2 * REACH + 1][p].start)
            when(even, near[REACH][p].start)

    when(wraps, lambda: facing_arrived(False))
    when(n_far_above > 0, lambda: pl.semaphore_wait(far_sem, n_far_above))
    sends(2)
    arrived = chunk_buf.at[pl.ds(1, cols - 1)]

    def reduce_chunks():
        pltpu.make_async_copy(arrived, arrived, group_sems.at[1]).wait()
        when(n_region_above > 0, lambda: pl.semaphore_wait(region_sem, n_region_above))
        reduced = up_send[jnp.clip(c - first_red, 0, n_red - 1)].astype(F32)
        for e in range(1, cols):
            reduced = reduced + chunk_buf[e].astype(F32)
        reduced_send[...] = reduced.astype(BF16)
        for d in range(REACH, rows):
            for e in range(cols):
                remote(
                    reduced_send, region_buf.at[d - REACH, c - first_red], group_sems.at[4], group_sems.at[5],
                    behind(d, e),
                ).start()

    def got(d, e):
        cell = d * REACH + e
        for p in range(pieces):
            near[cell][p].wait_recv()
            when(odd if d == 0 else even, near[REACH + e][p].start)
            if d == 0:
                when(last if e == 2 else end, around[e][p].start)
            if e == 2:
                when(jnp.logical_and(passes, c != cols - 2), near[cell - 1][p].start)

    when(is_red, reduce_chunks)
    when(jnp.logical_not(wraps), lambda: facing_arrived(True))

    def own_groups(lo, hi):
        for g in range(lo, hi):
            j, n = spans[g]
            view = leaf_buf.at[pl.ds(j, n)]
            pltpu.make_async_copy(view, view, own_sems.at[g]).wait()
            band_up[g].start()
            when(odd, band_across[g].start)

    def here(cell):
        for near_copy in near[cell]:
            near_copy.wait_recv()
        return term(cell)

    def up_groups():
        for g in range(len(spans)):
            band_up[g].wait_recv()
            when(even, band_across[g].start)

    def arrivals_last():
        own_groups(0, len(spans))
        got(0, 2)
        when(end, lambda: got(0, 1))
        up_groups()
        got(2, 2)

    def arrivals():
        own_groups(0, 1)
        start_all(near[2], wraps)
        start_all(first_to_end, c == 0)
        own_groups(1, len(spans))
        got(0, 2)
        got(2, 2)
        up_groups()

    when(last, arrivals_last)
    when(jnp.logical_not(last), arrivals)
    for cell in (2 * REACH, 2, 2 * REACH + 2):
        total = total + term(cell)
    total = total + here(REACH)
    when(jnp.logical_not(end), lambda: got(0, 1))
    total = total + term(1)

    pltpu.make_async_copy(region_buf, region_buf, group_sems.at[5]).wait()
    rank, vecs = leaf_buf.shape[1:]
    region_out = None
    for d in range(REACH, rows):
        target = lax.rem(r + d, rows)
        slot = jnp.int32(0)
        for f in range(rows):
            slot = jnp.where(list_ref[f] == target, f, slot)
        region = region_buf[d - REACH].astype(F32).reshape(rank, vecs).astype(BF16)
        product = dot(coupling[slot], region, ((0,), (0,)))
        region_out = product if region_out is None else region_out + product
    leaf_out = dot(transfer_row[...], region_out.astype(BF16), ((0,), (0,)))
    mid_band = leaf_buf.at[pl.ds(band, band)]
    pltpu.make_async_copy(mid_band, mid_band, group_sems.at[6]).wait()
    leaf_out = leaf_out + dot(
        couple[...].reshape(REACH * band * rank, rank),
        leaf_buf[...].reshape(REACH * band * rank, vecs),
        ((0,), (0,)),
    )
    total = total + dot(leaf_out.astype(BF16), basis_row[...], ((0,), (0,)))
    got(2, 1)
    total = total + term(2 * REACH + 1)
    total = total + here(REACH + 2)
    total = total + here(REACH + 1)
    out_ref[...] = total.astype(out_ref.dtype)

    def sent(cells):
        view = table.at[pl.ds(0, cells)]
        pltpu.make_async_copy(view, view, group_sems.at[2]).wait()

    n_sent = table.shape[0] - 1
    short = jnp.logical_or(c == near_reach - 1, c == cols - near_reach)
    when(short, lambda: sent(n_sent - 1))
    when(end, lambda: [sent(n_sent + 1), sent(1)])
    when(jnp.logical_not(jnp.logical_or(short, end)), lambda: sent(n_sent))
    pltpu.make_async_copy(leaf_buf, leaf_buf, group_sems.at[3]).wait()

    @pl.when(is_red)
    def _():
        others = up_send.at[pl.ds(1, n_red - 1)]
        pltpu.make_async_copy(others, others, group_sems.at[0]).wait()
        for d in range(REACH, rows):
            pltpu.make_async_copy(chunk_buf, chunk_buf, group_sems.at[4]).wait()

    @pl.when(jnp.logical_not(is_red))
    def _():
        pltpu.make_async_copy(up_send, up_send, group_sems.at[0]).wait()


def per_device(
    vectors,
    near_blocks,
    near_source,
    near_count,
    basis_col,
    transfer_col,
    leaf_couple,
    coupling,
    distant_region_list,
    transfer_row,
    basis_row,
):
    rows, cols = lax.axis_size("row"), lax.axis_size("col")
    vecs, leaf = vectors.shape[2:]
    rank = basis_col.shape[2]
    cells = near_blocks.shape[2]
    band = leaf_couple.shape[3]
    n_red = cols // 4
    groups = min(band, 5)
    groups = -(-band // -(-band // groups))
    hbm = pl.BlockSpec(memory_space=pl.ANY)
    out = pl.pallas_call(
        functools.partial(kernel, rows, cols),
        out_shape=pltpu.VMEM((vecs, leaf), BF16),
        in_specs=[hbm] * 11,
        out_specs=pl.BlockSpec(memory_space=pltpu.VMEM),
        scratch_shapes=[
            pltpu.SMEM((cells,), jnp.int32),
            pltpu.SMEM((1, 1), jnp.int32),
            pltpu.SMEM((rows,), jnp.int32),
            pltpu.VMEM((cells, vecs, leaf), BF16),
            pltpu.VMEM((cells, leaf, leaf), BF16),
            pltpu.VMEM((rank, leaf), BF16),
            pltpu.VMEM((rank, rank), BF16),
            pltpu.VMEM((REACH * band, rank, rank), BF16),
            pltpu.VMEM((rows, rank, rank), BF16),
            pltpu.VMEM((rank, rank), BF16),
            pltpu.VMEM((rank, leaf), BF16),
            pltpu.VMEM((rank, vecs), BF16),
            pltpu.VMEM((n_red, rank // n_red, vecs), BF16),
            pltpu.VMEM((rank // n_red, vecs), BF16),
            pltpu.VMEM((REACH * band, rank, vecs), BF16),
            pltpu.VMEM((cols, rank // n_red, vecs), BF16),
            pltpu.VMEM((rows - REACH, n_red, rank // n_red, vecs), BF16),
            pltpu.SemaphoreType.DMA((11,)),
            pltpu.SemaphoreType.DMA((cells - 1, PIECES)),
            pltpu.SemaphoreType.DMA((groups,)),
            pltpu.SemaphoreType.DMA((groups,)),
            pltpu.SemaphoreType.DMA((7,)),
            pltpu.SemaphoreType.REGULAR,
            pltpu.SemaphoreType.REGULAR,
            pltpu.SemaphoreType.REGULAR,
        ],
        compiler_params=pltpu.CompilerParams(collective_id=0, has_side_effects=True),
    )(
        near_source[0, 0],
        near_count,
        distant_region_list[0],
        vectors[0, 0],
        near_blocks[0, 0],
        basis_col[0, 0],
        transfer_col[0, 0],
        leaf_couple[0, 0].reshape(REACH * band, rank, rank),
        coupling[0],
        transfer_row[0, 0],
        basis_row[0, 0],
    )
    return out[None, None]


def solution(mesh):
    placed = (
        P("row", "col", None, None),
        P("row", "col", None, None, None),
        P("row", "col", None),
        P("row", "col"),
        P("row", "col", None, None),
        P("row", "col", None, None),
        P("row", "col", None, None, None, None),
        P("row", None, None, None),
        P("row", None),
        P("row", "col", None, None),
        P("row", "col", None, None),
    )
    return jax.shard_map(
        per_device,
        mesh=mesh,
        in_specs=placed,
        out_specs=P("row", "col", None, None),
        check_vma=False,
    )
```

```python
import functools

import jax
import jax.numpy as jnp
from jax import lax
from jax.experimental import pallas as pl
from jax.experimental.pallas import tpu as pltpu
from jax.sharding import PartitionSpec as P

REACH = 3
PIECES = 4
MESH = pl.DeviceIdType.MESH
BF16 = jnp.bfloat16
F32 = jnp.float32


def dot(a, b, dims):
    return lax.dot_general(a, b, (dims, ((), ())), preferred_element_type=F32)


def kernel(
    rows,
    cols,
    source_hbm,
    count_hbm,
    list_hbm,
    vectors_hbm,
    blocks_hbm,
    basis_col_hbm,
    transfer_col_hbm,
    couple_hbm,
    coupling_hbm,
    transfer_row_hbm,
    basis_row_hbm,
    out_ref,
    source_ref,
    count_ref,
    list_ref,
    table,
    blocks,
    basis_col,
    transfer_col,
    couple,
    coupling,
    transfer_row,
    basis_row,
    leaf_send,
    up_send,
    reduced_send,
    leaf_buf,
    chunk_buf,
    region_buf,
    local_sems,
    near_recv_sems,
    own_sems,
    up_recv_sems,
    group_sems,
    near_sem,
    far_sem,
    region_sem,
    facing_sem,
    go_sem,
):
    r, c = lax.axis_index("row"), lax.axis_index("col")
    parity = lax.rem(r, 2)
    band = cols - REACH
    near_reach = REACH - 1
    n_red, chunk = up_send.shape[0], up_send.shape[1]
    first_red = n_red
    is_red = jnp.logical_and(c >= first_red, c < first_red + n_red)

    def behind(d, e):
        return (lax.rem(r + rows - d, rows), lax.rem(c + cols - e, cols))

    def when(condition, act):
        @pl.when(condition)
        def _():
            act()

    loads = [
        pltpu.make_async_copy(src, dst, local_sems.at[i])
        for i, (src, dst) in enumerate(
            [
                (vectors_hbm, table.at[0]),
                (basis_col_hbm, basis_col),
                (transfer_col_hbm, transfer_col),
                (blocks_hbm, blocks),
                (couple_hbm, couple),
                (coupling_hbm, coupling),
                (transfer_row_hbm, transfer_row),
                (basis_row_hbm, basis_row),
                (source_hbm, source_ref),
                (count_hbm, count_ref),
                (list_hbm, list_ref),
            ]
        )
    ]
    for load in loads[:3]:
        load.start()

    barrier = pltpu.get_barrier_semaphore()

    def place(row, col):
        return ((row // 2 + col // 2 + lax.rem(col, 2)) * cols + col) * rows + row

    mine = place(r, c)

    def near_column(col):
        return jnp.abs(col - c) <= near_reach

    far_rows = rows - REACH
    one = jnp.bool_(True)

    def to_row(k):
        return one, behind(0, k + 1)

    def to_facing(k):
        return one, behind(rows - 2 + 4 * k if rows > 4 else 2, 0)

    def to_targets(k):
        return is_red, behind(REACH + k // cols, k % cols)

    def to_reducers(k):
        return one, (lax.rem(r + REACH + k // n_red, rows), first_red + k % n_red)

    kinds = [
        (cols - 1, to_row, near_column),
        (2 if rows > 4 else 1, to_facing, None),
        (far_rows * cols, to_targets, None),
        (far_rows * n_red, to_reducers, None),
    ]

    def greet(sem, device):
        pl.semaphore_signal(sem, inc=1, device_id=device, device_id_type=MESH)

    def greet_all(down):
        for number, which, is_near in kinds:

            def act(k, which=which, is_near=is_near):
                valid, device = which(k)
                if not down:
                    when(jnp.logical_and(valid, place(*device) > mine), functools.partial(greet, barrier, device))
                    return
                below = jnp.logical_and(valid, place(*device) < mine)
                if which is to_facing:
                    when(below, functools.partial(greet, facing_sem, device))
                if which is to_reducers:
                    when(below, functools.partial(greet, region_sem, device))
                if is_near is None:
                    return
                close = is_near(device[1])
                when(jnp.logical_and(below, close), functools.partial(greet, near_sem, device))
                when(jnp.logical_and(below, jnp.logical_not(close)), functools.partial(greet, far_sem, device))

            if number <= 16:
                for k in range(number):
                    act(k)
            else:
                pl.loop(0, number)(act)

    def count_all(numbers):
        for number, which, is_near in kinds:

            def add(k, numbers, which=which, is_near=is_near):
                valid, device = which(k)
                above = place(*device) > mine
                no = jnp.logical_not(one)
                if is_near is None:
                    found = (
                        jnp.logical_not(above), no, no,
                        above if which is to_targets else no, above if which is to_facing else no,
                    )
                else:
                    close = is_near(device[1])
                    found = (
                        jnp.logical_not(above),
                        jnp.logical_and(above, close),
                        jnp.logical_and(above, jnp.logical_not(close)),
                        no,
                        no,
                    )
                return tuple(n + jnp.where(jnp.logical_and(valid, f), 1, 0) for n, f in zip(numbers, found))

            if number <= 16:
                for k in range(number):
                    numbers = add(k, numbers)
            else:
                numbers = lax.fori_loop(0, number, add, numbers)
        return numbers

    greet(barrier, (r + 1 - 2 * parity, c))
    greet_all(False)
    zero = jnp.int32(0)
    n_below, n_near_above, n_far_above, n_region_above, n_facing_above = count_all((jnp.int32(1), zero, zero, zero, zero))

    for load in loads[3:]:
        load.start()
    pl.semaphore_wait(barrier, n_below)
    greet_all(True)
    for load in loads[:3]:
        load.wait()
    leaf_low = dot(basis_col[...], table[0], ((1,), (1,))).astype(BF16)
    leaf_send[...] = leaf_low
    up = dot(transfer_col[...], leaf_low, ((0,), (0,))).astype(BF16)
    for j in range(n_red):
        up_send[j] = up[j * chunk : (j + 1) * chunk]

    def remote(src, dst, send_sem, recv_sem, target):
        return pltpu.make_async_remote_copy(
            src_ref=src, dst_ref=dst, send_sem=send_sem, recv_sem=recv_sem,
            device_id=target, device_id_type=MESH,
        )

    side = lax.rem(c, 2)
    passes, direct = side == 0, side == 1
    partner = (r + 1 - 2 * parity, c)
    odd, even = parity == 1, parity == 0
    group = -(-band // own_sems.shape[0])
    spans = [(j, min(group, band - j)) for j in range(0, band, group)]

    pieces = near_recv_sems.shape[1]
    part = table.shape[1] // pieces

    def near_copies(source, cell, target):
        return [
            remote(
                table.at[source, pl.ds(p * part, part)], table.at[cell, pl.ds(p * part, part)],
                group_sems.at[2], near_recv_sems.at[cell - 1, p], target,
            )
            for p in range(pieces)
        ]

    beside = (r, c + 1 - 2 * side)
    near = {
        2 * REACH: near_copies(0, 2 * REACH, behind(2, 0)),
        2: near_copies(0, 2, behind(0, 2)),
        2 * REACH + 2: near_copies(2 * REACH, 2 * REACH + 2, behind(0, 2)),
    }
    last, end = c >= cols - near_reach, c == cols - 1
    around = {e: near_copies(e, 2 * REACH + e, behind(2, 0)) for e in (1, 2)}
    first_to_end = near_copies(0, 1, (r, cols - 1))
    for d in (0, 2):
        near[d * REACH + 1] = near_copies(d * REACH + 2 * (1 - side), d * REACH + 1, beside)
    for e in range(REACH):
        near[REACH + e] = near_copies(2 * REACH * (1 - parity) + e, REACH + e, partner)

    chunks = [
        remote(
            up_send.at[j],
            chunk_buf.at[lax.rem(c + cols - (first_red + j), cols)],
            group_sems.at[0],
            group_sems.at[1],
            (r, first_red + j),
        )
        for j in range(n_red)
    ]
    leaves = [
        remote(leaf_send, leaf_buf.at[j], group_sems.at[7], own_sems.at[j // group], behind(0, REACH + j))
        for j in range(band)
    ]
    band_up = [
        remote(
            leaf_buf.at[pl.ds(j, n)], leaf_buf.at[pl.ds(2 * band + j, n)],
            group_sems.at[3], up_recv_sems.at[j // group], behind(2, 0),
        )
        for j, n in spans
    ]
    band_across = [
        remote(
            leaf_buf.at[pl.ds(2 * band * (1 - parity) + j, n)], leaf_buf.at[pl.ds(band + j, n)],
            group_sems.at[3], group_sems.at[6], partner,
        )
        for j, n in spans
    ]

    def known(target, stage, is_near=None):
        below = place(*target) < mine
        if stage == 0:
            return below
        close = near_column(target[1])
        return jnp.logical_and(jnp.logical_not(below), close if stage == 1 else jnp.logical_not(close))

    def start_all(copies, condition):
        for copy in copies:
            when(condition, copy.start)

    def sends(stage):
        for j in range(n_red):
            target = (r, first_red + j)
            when(jnp.logical_and(known(target, stage), target[1] != c), chunks[j].start)
        for j in range(band):
            when(known(behind(0, REACH + j), stage), leaves[j].start)
        if stage != 2:
            start_all(near[2], known(behind(0, 2), stage))
        if stage == 0:
            start_all(near[1], direct)
        if stage == 0:
            start_all(near[2 * REACH], known(behind(2, 0), stage))

    sends(0)
    when(n_facing_above > 0, lambda: pl.semaphore_wait(facing_sem, n_facing_above))
    start_all(near[2 * REACH], jnp.logical_not(known(behind(2, 0), 0)))
    when(n_near_above > 0, lambda: pl.semaphore_wait(near_sem, n_near_above))
    sends(1)

    for near_copy in near[REACH]:
        when(odd, near_copy.start)
    for load in loads[3:]:
        load.wait()

    count = count_ref[0, 0]

    sources = [source_ref[s] for s in range(source_ref.shape[0])]
    slots = []
    for cell in range(len(sources)):
        slot = jnp.int32(0)
        for s, source in enumerate(sources):
            slot = jnp.where(source == cell, s, slot)
        slots.append(slot)

    def term(cell):
        slot = slots[cell]
        source = table[cell]
        source = jnp.where(slot < count, source, jnp.zeros_like(source))
        return dot(source, blocks[slot], ((1,), (0,)))

    total = term(0)
    wraps = known(behind(0, 2), 2)

    def facing_arrived(pass_on):
        for p in range(pieces):
            near[2 * REACH][p].wait_recv()
            if pass_on:
                near[2 * REACH + 2][p].start()
            when(direct, near[2 * REACH + 1][p].start)
            when(even, near[REACH][p].start)

    when(wraps, lambda: facing_arrived(False))
    when(n_far_above > 0, lambda: pl.semaphore_wait(far_sem, n_far_above))
    sends(2)

    follows = jnp.logical_and(c >= near_reach, c < 2 * near_reach)
    own_band = leaf_buf.at[pl.ds(0, band)]

    def leaves_sent():
        pltpu.make_async_copy(own_band, own_band, group_sems.at[7]).wait()

    def release():
        leaves_sent()
        greet(go_sem, (r, lax.rem(c + cols - near_reach, cols)))

    when(follows, release)

    def wrap():
        pl.semaphore_wait(go_sem, 1)
        start_all(near[2], one)
        start_all(first_to_end, c == 0)

    when(c == 1, wrap)
    arrived = chunk_buf.at[pl.ds(1, cols - 1)]

    def reduce_chunks():
        pltpu.make_async_copy(arrived, arrived, group_sems.at[1]).wait()
        when(n_region_above > 0, lambda: pl.semaphore_wait(region_sem, n_region_above))
        reduced = up_send[jnp.clip(c - first_red, 0, n_red - 1)].astype(F32)
        for e in range(1, cols):
            reduced = reduced + chunk_buf[e].astype(F32)
        reduced_send[...] = reduced.astype(BF16)
        for d in range(REACH, rows):
            for e in range(cols):
                remote(
                    reduced_send, region_buf.at[d - REACH, c - first_red], group_sems.at[4], group_sems.at[5],
                    behind(d, e),
                ).start()

    def got(d, e):
        cell = d * REACH + e
        for p in range(pieces):
            near[cell][p].wait_recv()
            when(odd if d == 0 else even, near[REACH + e][p].start)
            if d == 0:
                when(last if e == 2 else end, around[e][p].start)
            if e == 2:
                when(jnp.logical_and(passes, c != cols - 2), near[cell - 1][p].start)

    when(is_red, reduce_chunks)
    when(jnp.logical_not(wraps), lambda: facing_arrived(True))

    def own_groups(lo, hi):
        for g in range(lo, hi):
            j, n = spans[g]
            view = leaf_buf.at[pl.ds(j, n)]
            pltpu.make_async_copy(view, view, own_sems.at[g]).wait()
            band_up[g].start()
            when(odd, band_across[g].start)

    def here(cell):
        for near_copy in near[cell]:
            near_copy.wait_recv()
        return term(cell)

    def up_groups():
        for g in range(len(spans)):
            band_up[g].wait_recv()
            when(even, band_across[g].start)

    own_groups(0, 1)
    when(c == 0, wrap)
    own_groups(1, len(spans))
    got(0, 2)
    when(end, lambda: got(0, 1))

    def from_beside():
        got(0, 1)
        got(2, 1)

    when(passes, from_beside)
    when(jnp.logical_not(last), lambda: got(2, 2))
    for cell in (2 * REACH, 2):
        total = total + term(cell)
    up_groups()
    when(last, lambda: got(2, 2))
    total = total + term(2 * REACH + 2)
    total = total + here(REACH)
    when(jnp.logical_and(direct, jnp.logical_not(end)), lambda: got(0, 1))
    total = total + term(1)

    pltpu.make_async_copy(region_buf, region_buf, group_sems.at[5]).wait()
    rank, vecs = leaf_buf.shape[1:]
    region_out = None
    for d in range(REACH, rows):
        target = lax.rem(r + d, rows)
        slot = jnp.int32(0)
        for f in range(rows):
            slot = jnp.where(list_ref[f] == target, f, slot)
        region = region_buf[d - REACH].astype(F32).reshape(rank, vecs).astype(BF16)
        product = dot(coupling[slot], region, ((0,), (0,)))
        region_out = product if region_out is None else region_out + product
    leaf_out = dot(transfer_row[...], region_out.astype(BF16), ((0,), (0,)))
    mid_band = leaf_buf.at[pl.ds(band, band)]
    pltpu.make_async_copy(mid_band, mid_band, group_sems.at[6]).wait()
    leaf_out = leaf_out + dot(
        couple[...].reshape(REACH * band * rank, rank),
        leaf_buf[...].reshape(REACH * band * rank, vecs),
        ((0,), (0,)),
    )
    total = total + dot(leaf_out.astype(BF16), basis_row[...], ((0,), (0,)))
    when(direct, lambda: got(2, 1))
    total = total + term(2 * REACH + 1)
    total = total + here(REACH + 2)
    total = total + here(REACH + 1)
    out_ref[...] = total.astype(out_ref.dtype)

    def sent(cells):
        view = table.at[pl.ds(0, cells)]
        pltpu.make_async_copy(view, view, group_sems.at[2]).wait()

    n_sent = table.shape[0] - 1
    short = jnp.logical_or(c == near_reach - 1, c == cols - near_reach)
    when(short, lambda: sent(n_sent - 1))
    when(end, lambda: [sent(n_sent + 1), sent(1)])
    when(jnp.logical_not(jnp.logical_or(short, end)), lambda: sent(n_sent))
    upper_bands = leaf_buf.at[pl.ds(band, 2 * band)]
    pltpu.make_async_copy(upper_bands, upper_bands, group_sems.at[3]).wait()
    when(jnp.logical_not(follows), leaves_sent)

    @pl.when(is_red)
    def _():
        others = up_send.at[pl.ds(1, n_red - 1)]
        pltpu.make_async_copy(others, others, group_sems.at[0]).wait()
        for d in range(REACH, rows):
            pltpu.make_async_copy(chunk_buf, chunk_buf, group_sems.at[4]).wait()

    @pl.when(jnp.logical_not(is_red))
    def _():
        pltpu.make_async_copy(up_send, up_send, group_sems.at[0]).wait()


def per_device(
    vectors,
    near_blocks,
    near_source,
    near_count,
    basis_col,
    transfer_col,
    leaf_couple,
    coupling,
    distant_region_list,
    transfer_row,
    basis_row,
):
    rows, cols = lax.axis_size("row"), lax.axis_size("col")
    vecs, leaf = vectors.shape[2:]
    rank = basis_col.shape[2]
    cells = near_blocks.shape[2]
    band = leaf_couple.shape[3]
    n_red = cols // 4
    groups = min(band, 5)
    groups = -(-band // -(-band // groups))
    hbm = pl.BlockSpec(memory_space=pl.ANY)
    out = pl.pallas_call(
        functools.partial(kernel, rows, cols),
        out_shape=pltpu.VMEM((vecs, leaf), BF16),
        in_specs=[hbm] * 11,
        out_specs=pl.BlockSpec(memory_space=pltpu.VMEM),
        scratch_shapes=[
            pltpu.SMEM((cells,), jnp.int32),
            pltpu.SMEM((1, 1), jnp.int32),
            pltpu.SMEM((rows,), jnp.int32),
            pltpu.VMEM((cells, vecs, leaf), BF16),
            pltpu.VMEM((cells, leaf, leaf), BF16),
            pltpu.VMEM((rank, leaf), BF16),
            pltpu.VMEM((rank, rank), BF16),
            pltpu.VMEM((REACH * band, rank, rank), BF16),
            pltpu.VMEM((rows, rank, rank), BF16),
            pltpu.VMEM((rank, rank), BF16),
            pltpu.VMEM((rank, leaf), BF16),
            pltpu.VMEM((rank, vecs), BF16),
            pltpu.VMEM((n_red, rank // n_red, vecs), BF16),
            pltpu.VMEM((rank // n_red, vecs), BF16),
            pltpu.VMEM((REACH * band, rank, vecs), BF16),
            pltpu.VMEM((cols, rank // n_red, vecs), BF16),
            pltpu.VMEM((rows - REACH, n_red, rank // n_red, vecs), BF16),
            pltpu.SemaphoreType.DMA((11,)),
            pltpu.SemaphoreType.DMA((cells - 1, PIECES)),
            pltpu.SemaphoreType.DMA((groups,)),
            pltpu.SemaphoreType.DMA((groups,)),
            pltpu.SemaphoreType.DMA((8,)),
            pltpu.SemaphoreType.REGULAR,
            pltpu.SemaphoreType.REGULAR,
            pltpu.SemaphoreType.REGULAR,
            pltpu.SemaphoreType.REGULAR,
            pltpu.SemaphoreType.REGULAR,
        ],
        compiler_params=pltpu.CompilerParams(collective_id=0, has_side_effects=True),
    )(
        near_source[0, 0],
        near_count,
        distant_region_list[0],
        vectors[0, 0],
        near_blocks[0, 0],
        basis_col[0, 0],
        transfer_col[0, 0],
        leaf_couple[0, 0].reshape(REACH * band, rank, rank),
        coupling[0],
        transfer_row[0, 0],
        basis_row[0, 0],
    )
    return out[None, None]


def solution(mesh):
    placed = (
        P("row", "col", None, None),
        P("row", "col", None, None, None),
        P("row", "col", None),
        P("row", "col"),
        P("row", "col", None, None),
        P("row", "col", None, None),
        P("row", "col", None, None, None, None),
        P("row", None, None, None),
        P("row", None),
        P("row", "col", None, None),
        P("row", "col", None, None),
    )
    return jax.shard_map(
        per_device,
        mesh=mesh,
        in_specs=placed,
        out_specs=P("row", "col", None, None),
        check_vma=False,
    )
```

```python
import functools

import jax
import jax.numpy as jnp
from jax import lax
from jax.experimental import pallas as pl
from jax.experimental.pallas import tpu as pltpu
from jax.sharding import PartitionSpec as P

REACH = 3
PIECES = 4
MESH = pl.DeviceIdType.MESH
BF16 = jnp.bfloat16
F32 = jnp.float32


def dot(a, b, dims):
    return lax.dot_general(a, b, (dims, ((), ())), preferred_element_type=F32)


def kernel(
    rows,
    cols,
    source_hbm,
    count_hbm,
    list_hbm,
    vectors_hbm,
    blocks_hbm,
    basis_col_hbm,
    transfer_col_hbm,
    couple_hbm,
    coupling_hbm,
    transfer_row_hbm,
    basis_row_hbm,
    out_ref,
    source_ref,
    count_ref,
    list_ref,
    table,
    blocks,
    basis_col,
    transfer_col,
    couple,
    coupling,
    transfer_row,
    basis_row,
    leaf_send,
    up_send,
    reduced_send,
    leaf_buf,
    chunk_buf,
    region_buf,
    local_sems,
    near_recv_sems,
    own_sems,
    up_recv_sems,
    group_sems,
    near_sem,
    far_sem,
    region_sem,
    facing_sem,
    go_sem,
):
    r, c = lax.axis_index("row"), lax.axis_index("col")
    parity = lax.rem(r, 2)
    band = cols - REACH
    near_reach = REACH - 1
    n_red, chunk = up_send.shape[0], up_send.shape[1]
    first_red = n_red
    is_red = jnp.logical_and(c >= first_red, c < first_red + n_red)

    def behind(d, e):
        return (lax.rem(r + rows - d, rows), lax.rem(c + cols - e, cols))

    def when(condition, act):
        @pl.when(condition)
        def _():
            act()

    loads = [
        pltpu.make_async_copy(src, dst, local_sems.at[min(i, 3)])
        for i, (src, dst) in enumerate(
            [
                (vectors_hbm, table.at[0]),
                (basis_col_hbm, basis_col),
                (transfer_col_hbm, transfer_col),
                (blocks_hbm, blocks),
                (couple_hbm, couple),
                (coupling_hbm, coupling),
                (transfer_row_hbm, transfer_row),
                (basis_row_hbm, basis_row),
                (source_hbm, source_ref),
                (count_hbm, count_ref),
                (list_hbm, list_ref),
            ]
        )
    ]
    for load in loads[:3]:
        load.start()

    barrier = pltpu.get_barrier_semaphore()

    def place(row, col):
        return ((row // 2 + col // 2 + lax.rem(col, 2)) * cols + col) * rows + row

    mine = place(r, c)

    def near_column(col):
        return jnp.abs(col - c) <= near_reach

    far_rows = rows - REACH
    one = jnp.bool_(True)

    def to_row(k):
        return one, behind(0, k + 1)

    def to_facing(k):
        return one, behind(rows - 2 + 4 * k if rows > 4 else 2, 0)

    def to_targets(k):
        return is_red, behind(REACH + k // cols, k % cols)

    def to_reducers(k):
        return one, (lax.rem(r + REACH + k // n_red, rows), first_red + k % n_red)

    kinds = [
        (cols - 1, to_row, near_column),
        (2 if rows > 4 else 1, to_facing, None),
        (far_rows * cols, to_targets, None),
        (far_rows * n_red, to_reducers, None),
    ]

    def greet(sem, device):
        pl.semaphore_signal(sem, inc=1, device_id=device, device_id_type=MESH)

    def greet_all(down):
        for number, which, is_near in kinds:

            def act(k, which=which, is_near=is_near):
                valid, device = which(k)
                if not down:
                    when(jnp.logical_and(valid, place(*device) > mine), functools.partial(greet, barrier, device))
                    return
                below = jnp.logical_and(valid, place(*device) < mine)
                if which is to_facing:
                    when(below, functools.partial(greet, facing_sem, device))
                if which is to_reducers:
                    when(below, functools.partial(greet, region_sem, device))
                if is_near is None:
                    return
                close = is_near(device[1])
                when(jnp.logical_and(below, close), functools.partial(greet, near_sem, device))
                when(jnp.logical_and(below, jnp.logical_not(close)), functools.partial(greet, far_sem, device))

            if number <= 16:
                for k in range(number):
                    act(k)
            else:
                pl.loop(0, number)(act)

    def count_all(numbers):
        for number, which, is_near in kinds:

            def add(k, numbers, which=which, is_near=is_near):
                valid, device = which(k)
                above = place(*device) > mine
                no = jnp.logical_not(one)
                if is_near is None:
                    found = (
                        jnp.logical_not(above), no, no,
                        above if which is to_targets else no, above if which is to_facing else no,
                    )
                else:
                    close = is_near(device[1])
                    found = (
                        jnp.logical_not(above),
                        jnp.logical_and(above, close),
                        jnp.logical_and(above, jnp.logical_not(close)),
                        no,
                        no,
                    )
                return tuple(n + jnp.where(jnp.logical_and(valid, f), 1, 0) for n, f in zip(numbers, found))

            if number <= 16:
                for k in range(number):
                    numbers = add(k, numbers)
            else:
                numbers = lax.fori_loop(0, number, add, numbers)
        return numbers

    greet(barrier, (r + 1 - 2 * parity, c))
    greet_all(False)
    zero = jnp.int32(0)
    n_below, n_near_above, n_far_above, n_region_above, n_facing_above = count_all((jnp.int32(1), zero, zero, zero, zero))

    for load in loads[3:]:
        load.start()
    pl.semaphore_wait(barrier, n_below)
    greet_all(True)
    for load in loads[:3]:
        load.wait()
    leaf_low = dot(basis_col[...], table[0], ((1,), (1,))).astype(BF16)
    leaf_send[...] = leaf_low
    up = dot(transfer_col[...], leaf_low, ((0,), (0,))).astype(BF16)
    for j in range(n_red):
        up_send[j] = up[j * chunk : (j + 1) * chunk]

    def remote(src, dst, send_sem, recv_sem, target):
        return pltpu.make_async_remote_copy(
            src_ref=src, dst_ref=dst, send_sem=send_sem, recv_sem=recv_sem,
            device_id=target, device_id_type=MESH,
        )

    side = lax.rem(c, 2)
    passes, direct = side == 0, side == 1
    partner = (r + 1 - 2 * parity, c)
    odd, even = parity == 1, parity == 0
    group = -(-band // own_sems.shape[0])
    spans = [(j, min(group, band - j)) for j in range(0, band, group)]

    pieces = near_recv_sems.shape[1]
    part = table.shape[1] // pieces

    def near_copies(source, cell, target):
        return [
            remote(
                table.at[source, pl.ds(p * part, part)], table.at[cell, pl.ds(p * part, part)],
                group_sems.at[2],
                group_sems.at[5 + cell] if REACH <= cell < 2 * REACH else near_recv_sems.at[cell - 1 - (REACH if cell > 2 else 0), p],
                target,
            )
            for p in range(pieces)
        ]

    beside = (r, c + 1 - 2 * side)
    near = {
        2 * REACH: near_copies(0, 2 * REACH, behind(2, 0)),
        2: near_copies(0, 2, behind(0, 2)),
        2 * REACH + 2: near_copies(2 * REACH, 2 * REACH + 2, behind(0, 2)),
    }
    last, end = c >= cols - near_reach, c == cols - 1
    around = {e: near_copies(e, 2 * REACH + e, behind(2, 0)) for e in (1, 2)}
    first_to_end = near_copies(0, 1, (r, cols - 1))
    for d in (0, 2):
        near[d * REACH + 1] = near_copies(d * REACH + 2 * (1 - side), d * REACH + 1, beside)
    for e in range(REACH):
        near[REACH + e] = near_copies(2 * REACH * (1 - parity) + e, REACH + e, partner)

    chunks = [
        remote(
            up_send.at[j],
            chunk_buf.at[lax.rem(c + cols - (first_red + j), cols)],
            group_sems.at[0],
            group_sems.at[1],
            (r, first_red + j),
        )
        for j in range(n_red)
    ]
    leaves = [
        remote(leaf_send, leaf_buf.at[j], group_sems.at[7], own_sems.at[j // group], behind(0, REACH + j))
        for j in range(band)
    ]
    band_up = [
        remote(
            leaf_buf.at[pl.ds(j, n)], leaf_buf.at[pl.ds(2 * band + j, n)],
            group_sems.at[3], up_recv_sems.at[j // group], behind(2, 0),
        )
        for j, n in spans
    ]
    band_across = [
        remote(
            leaf_buf.at[pl.ds(2 * band * (1 - parity) + j, n)], leaf_buf.at[pl.ds(band + j, n)],
            group_sems.at[3], group_sems.at[6], partner,
        )
        for j, n in spans
    ]

    def known(target, stage, is_near=None):
        below = place(*target) < mine
        if stage == 0:
            return below
        close = near_column(target[1])
        return jnp.logical_and(jnp.logical_not(below), close if stage == 1 else jnp.logical_not(close))

    def start_all(copies, condition):
        for copy in copies:
            when(condition, copy.start)

    def sends(stage):
        for j in range(n_red):
            target = (r, first_red + j)
            when(jnp.logical_and(known(target, stage), target[1] != c), chunks[j].start)
        for j in range(band):
            when(known(behind(0, REACH + j), stage), leaves[j].start)
        if stage != 2:
            start_all(near[2], known(behind(0, 2), stage))
        if stage == 0:
            start_all(near[1], direct)
        if stage == 0:
            start_all(near[2 * REACH], known(behind(2, 0), stage))

    sends(0)
    when(n_facing_above > 0, lambda: pl.semaphore_wait(facing_sem, n_facing_above))
    start_all(near[2 * REACH], jnp.logical_not(known(behind(2, 0), 0)))
    when(n_near_above > 0, lambda: pl.semaphore_wait(near_sem, n_near_above))
    sends(1)

    for near_copy in near[REACH]:
        when(odd, near_copy.start)
    for load in loads[3:]:
        load.wait()

    count = count_ref[0, 0]

    sources = [source_ref[s] for s in range(source_ref.shape[0])]
    slots = []
    for cell in range(len(sources)):
        slot = jnp.int32(0)
        for s, source in enumerate(sources):
            slot = jnp.where(source == cell, s, slot)
        slots.append(slot)

    def term(cell):
        slot = slots[cell]
        source = table[cell]
        source = jnp.where(slot < count, source, jnp.zeros_like(source))
        return dot(source, blocks[slot], ((1,), (0,)))

    total = term(0)
    wraps = known(behind(0, 2), 2)

    def facing_arrived(pass_on):
        for p in range(pieces):
            near[2 * REACH][p].wait_recv()
            if pass_on:
                near[2 * REACH + 2][p].start()
            when(direct, near[2 * REACH + 1][p].start)
            when(even, near[REACH][p].start)

    when(wraps, lambda: facing_arrived(False))
    when(n_far_above > 0, lambda: pl.semaphore_wait(far_sem, n_far_above))
    sends(2)

    follows = jnp.logical_and(c >= near_reach, c < 2 * near_reach)
    own_band = leaf_buf.at[pl.ds(0, band)]

    def leaves_sent():
        pltpu.make_async_copy(own_band, own_band, group_sems.at[7]).wait()

    def release():
        leaves_sent()
        greet(go_sem, (r, lax.rem(c + cols - near_reach, cols)))

    when(follows, release)

    def wrap():
        pl.semaphore_wait(go_sem, 1)
        start_all(near[2], one)
        start_all(first_to_end, c == 0)

    when(c == 1, wrap)
    arrived = chunk_buf.at[pl.ds(1, cols - 1)]

    def reduce_chunks():
        pltpu.make_async_copy(arrived, arrived, group_sems.at[1]).wait()
        when(n_region_above > 0, lambda: pl.semaphore_wait(region_sem, n_region_above))
        reduced = up_send[jnp.clip(c - first_red, 0, n_red - 1)].astype(F32)
        for e in range(1, cols):
            reduced = reduced + chunk_buf[e].astype(F32)
        reduced_send[...] = reduced.astype(BF16)
        for d in range(REACH, rows):
            for e in range(cols):
                remote(
                    reduced_send, region_buf.at[d - REACH, c - first_red], group_sems.at[4], group_sems.at[5],
                    behind(d, e),
                ).start()

    def got(d, e):
        cell = d * REACH + e
        for p in range(pieces):
            near[cell][p].wait_recv()
            when(odd if d == 0 else even, near[REACH + e][p].start)
            if d == 0:
                when(last if e == 2 else end, around[e][p].start)
            if e == 2:
                on = jnp.logical_and(passes, c != cols - 2)
                when(jnp.logical_and(on, odd) if d == 0 else on, near[cell - 1][p].start)
        if (d, e) == (2, 2):
            start_all(near[1], jnp.logical_and(on, even))

    when(is_red, reduce_chunks)
    when(jnp.logical_not(wraps), lambda: facing_arrived(True))

    def own_groups(lo, hi):
        for g in range(lo, hi):
            j, n = spans[g]
            view = leaf_buf.at[pl.ds(j, n)]
            pltpu.make_async_copy(view, view, own_sems.at[g]).wait()
            band_up[g].start()
            when(odd, band_across[g].start)

    def here(cell):
        view = table.at[cell]
        pltpu.make_async_copy(view, view, group_sems.at[5 + cell]).wait()
        return term(cell)

    def up_groups():
        for g in range(len(spans)):
            band_up[g].wait_recv()
            when(even, band_across[g].start)

    own_groups(0, 1)
    when(c == 0, wrap)
    own_groups(1, len(spans))
    got(0, 2)
    when(end, lambda: got(0, 1))

    def from_beside():
        got(0, 1)
        got(2, 1)

    when(passes, from_beside)
    when(jnp.logical_not(last), lambda: got(2, 2))
    for cell in (2 * REACH, 2):
        total = total + term(cell)
    up_groups()
    when(last, lambda: got(2, 2))
    total = total + term(2 * REACH + 2)
    total = total + here(REACH)
    inner = jnp.logical_and(direct, jnp.logical_not(end))
    when(jnp.logical_and(inner, odd), lambda: got(0, 1))

    pltpu.make_async_copy(region_buf, region_buf, group_sems.at[5]).wait()
    rank, vecs = leaf_buf.shape[1:]
    region_out = None
    for d in range(REACH, rows):
        target = lax.rem(r + d, rows)
        slot = jnp.int32(0)
        for f in range(rows):
            slot = jnp.where(list_ref[f] == target, f, slot)
        region = region_buf[d - REACH].astype(F32).reshape(rank, vecs).astype(BF16)
        product = dot(coupling[slot], region, ((0,), (0,)))
        region_out = product if region_out is None else region_out + product
    leaf_out = dot(transfer_row[...], region_out.astype(BF16), ((0,), (0,)))
    mid_band = leaf_buf.at[pl.ds(band, band)]
    pltpu.make_async_copy(mid_band, mid_band, group_sems.at[6]).wait()
    leaf_out = leaf_out + dot(
        couple[...].reshape(REACH * band * rank, rank),
        leaf_buf[...].reshape(REACH * band * rank, vecs),
        ((0,), (0,)),
    )
    total = total + dot(leaf_out.astype(BF16), basis_row[...], ((0,), (0,)))
    when(direct, lambda: got(2, 1))
    total = total + term(2 * REACH + 1)
    total = total + here(REACH + 2)
    when(jnp.logical_and(inner, even), lambda: got(0, 1))
    total = total + term(1)
    total = total + here(REACH + 1)
    out_ref[...] = total.astype(out_ref.dtype)

    def sent(cells):
        view = table.at[pl.ds(0, cells)]
        pltpu.make_async_copy(view, view, group_sems.at[2]).wait()

    n_sent = table.shape[0] - 1
    short = jnp.logical_or(c == near_reach - 1, c == cols - near_reach)
    when(short, lambda: sent(n_sent - 1))
    when(end, lambda: [sent(n_sent + 1), sent(1)])
    when(jnp.logical_not(jnp.logical_or(short, end)), lambda: sent(n_sent))
    upper_bands = leaf_buf.at[pl.ds(band, 2 * band)]
    pltpu.make_async_copy(upper_bands, upper_bands, group_sems.at[3]).wait()
    when(jnp.logical_not(follows), leaves_sent)

    @pl.when(is_red)
    def _():
        others = up_send.at[pl.ds(1, n_red - 1)]
        pltpu.make_async_copy(others, others, group_sems.at[0]).wait()
        for d in range(REACH, rows):
            pltpu.make_async_copy(chunk_buf, chunk_buf, group_sems.at[4]).wait()

    @pl.when(jnp.logical_not(is_red))
    def _():
        pltpu.make_async_copy(up_send, up_send, group_sems.at[0]).wait()


def per_device(
    vectors,
    near_blocks,
    near_source,
    near_count,
    basis_col,
    transfer_col,
    leaf_couple,
    coupling,
    distant_region_list,
    transfer_row,
    basis_row,
):
    rows, cols = lax.axis_size("row"), lax.axis_size("col")
    vecs, leaf = vectors.shape[2:]
    rank = basis_col.shape[2]
    cells = near_blocks.shape[2]
    band = leaf_couple.shape[3]
    n_red = cols // 4
    groups = min(band, 5)
    groups = -(-band // -(-band // groups))
    hbm = pl.BlockSpec(memory_space=pl.ANY)
    out = pl.pallas_call(
        functools.partial(kernel, rows, cols),
        out_shape=pltpu.VMEM((vecs, leaf), BF16),
        in_specs=[hbm] * 11,
        out_specs=pl.BlockSpec(memory_space=pltpu.VMEM),
        scratch_shapes=[
            pltpu.SMEM((cells,), jnp.int32),
            pltpu.SMEM((1, 1), jnp.int32),
            pltpu.SMEM((rows,), jnp.int32),
            pltpu.VMEM((cells, vecs, leaf), BF16),
            pltpu.VMEM((cells, leaf, leaf), BF16),
            pltpu.VMEM((rank, leaf), BF16),
            pltpu.VMEM((rank, rank), BF16),
            pltpu.VMEM((REACH * band, rank, rank), BF16),
            pltpu.VMEM((rows, rank, rank), BF16),
            pltpu.VMEM((rank, rank), BF16),
            pltpu.VMEM((rank, leaf), BF16),
            pltpu.VMEM((rank, vecs), BF16),
            pltpu.VMEM((n_red, rank // n_red, vecs), BF16),
            pltpu.VMEM((rank // n_red, vecs), BF16),
            pltpu.VMEM((REACH * band, rank, vecs), BF16),
            pltpu.VMEM((cols, rank // n_red, vecs), BF16),
            pltpu.VMEM((rows - REACH, n_red, rank // n_red, vecs), BF16),
            pltpu.SemaphoreType.DMA((4,)),
            pltpu.SemaphoreType.DMA((cells - 1 - REACH, PIECES)),
            pltpu.SemaphoreType.DMA((groups,)),
            pltpu.SemaphoreType.DMA((groups,)),
            pltpu.SemaphoreType.DMA((8 + REACH,)),
            pltpu.SemaphoreType.REGULAR,
            pltpu.SemaphoreType.REGULAR,
            pltpu.SemaphoreType.REGULAR,
            pltpu.SemaphoreType.REGULAR,
            pltpu.SemaphoreType.REGULAR,
        ],
        compiler_params=pltpu.CompilerParams(collective_id=0, has_side_effects=True),
    )(
        near_source[0, 0],
        near_count,
        distant_region_list[0],
        vectors[0, 0],
        near_blocks[0, 0],
        basis_col[0, 0],
        transfer_col[0, 0],
        leaf_couple[0, 0].reshape(REACH * band, rank, rank),
        coupling[0],
        transfer_row[0, 0],
        basis_row[0, 0],
    )
    return out[None, None]


def solution(mesh):
    placed = (
        P("row", "col", None, None),
        P("row", "col", None, None, None),
        P("row", "col", None),
        P("row", "col"),
        P("row", "col", None, None),
        P("row", "col", None, None),
        P("row", "col", None, None, None, None),
        P("row", None, None, None),
        P("row", None),
        P("row", "col", None, None),
        P("row", "col", None, None),
    )
    return jax.shard_map(
        per_device,
        mesh=mesh,
        in_specs=placed,
        out_specs=P("row", "col", None, None),
        check_vma=False,
    )
```

```python
import functools

import jax
import jax.numpy as jnp
from jax import lax
from jax.experimental import pallas as pl
from jax.experimental.pallas import tpu as pltpu
from jax.sharding import PartitionSpec as P

REACH = 3
PIECES = 4
MESH = pl.DeviceIdType.MESH
BF16 = jnp.bfloat16
F32 = jnp.float32


def dot(a, b, dims):
    return lax.dot_general(a, b, (dims, ((), ())), preferred_element_type=F32)


def kernel(
    rows,
    cols,
    source_hbm,
    count_hbm,
    list_hbm,
    vectors_hbm,
    blocks_hbm,
    basis_col_hbm,
    transfer_col_hbm,
    couple_hbm,
    coupling_hbm,
    transfer_row_hbm,
    basis_row_hbm,
    out_ref,
    source_ref,
    count_ref,
    list_ref,
    table,
    blocks,
    basis_col,
    transfer_col,
    couple,
    coupling,
    transfer_row,
    basis_row,
    leaf_send,
    up_send,
    reduced_send,
    leaf_buf,
    chunk_buf,
    region_buf,
    local_sems,
    near_recv_sems,
    own_sems,
    up_recv_sems,
    group_sems,
    near_sem,
    far_sem,
    region_sem,
    facing_sem,
    go_sem,
):
    r, c = lax.axis_index("row"), lax.axis_index("col")
    parity = lax.rem(r, 2)
    band = cols - REACH
    near_reach = REACH - 1
    n_red, chunk = up_send.shape[0], up_send.shape[1]
    first_red = n_red
    is_red = jnp.logical_and(c >= first_red, c < first_red + n_red)

    def behind(d, e):
        return (lax.rem(r + rows - d, rows), lax.rem(c + cols - e, cols))

    def when(condition, act):
        @pl.when(condition)
        def _():
            act()

    loads = [
        pltpu.make_async_copy(src, dst, local_sems.at[min(i, 3)])
        for i, (src, dst) in enumerate(
            [
                (vectors_hbm, table.at[0]),
                (basis_col_hbm, basis_col),
                (transfer_col_hbm, transfer_col),
                (blocks_hbm, blocks),
                (couple_hbm, couple),
                (coupling_hbm, coupling),
                (transfer_row_hbm, transfer_row),
                (basis_row_hbm, basis_row),
                (source_hbm, source_ref),
                (count_hbm, count_ref),
                (list_hbm, list_ref),
            ]
        )
    ]
    for load in loads[:3]:
        load.start()

    barrier = pltpu.get_barrier_semaphore()

    def place(row, col):
        return ((row // 2 + col // 2 + lax.rem(col, 2)) * cols + col) * rows + row

    mine = place(r, c)

    def near_column(col):
        return jnp.abs(col - c) <= near_reach

    far_rows = rows - REACH
    one = jnp.bool_(True)

    def to_row(k):
        return one, behind(0, k + 1)

    def to_facing(k):
        return one, behind(rows - 2 + 4 * k if rows > 4 else 2, 0)

    def to_targets(k):
        return is_red, behind(REACH + k // cols, k % cols)

    def to_reducers(k):
        return one, (lax.rem(r + REACH + k // n_red, rows), first_red + k % n_red)

    kinds = [
        (cols - 1, to_row, near_column),
        (2 if rows > 4 else 1, to_facing, None),
        (far_rows * cols, to_targets, None),
        (far_rows * n_red, to_reducers, None),
    ]

    def greet(sem, device):
        pl.semaphore_signal(sem, inc=1, device_id=device, device_id_type=MESH)

    def greet_all(down):
        for number, which, is_near in kinds:

            def act(k, which=which, is_near=is_near):
                valid, device = which(k)
                if not down:
                    when(jnp.logical_and(valid, place(*device) > mine), functools.partial(greet, barrier, device))
                    return
                below = jnp.logical_and(valid, place(*device) < mine)
                if which is to_facing:
                    when(below, functools.partial(greet, facing_sem, device))
                if which is to_reducers:
                    when(below, functools.partial(greet, region_sem, device))
                if is_near is None:
                    return
                close = is_near(device[1])
                when(jnp.logical_and(below, close), functools.partial(greet, near_sem, device))
                when(jnp.logical_and(below, jnp.logical_not(close)), functools.partial(greet, far_sem, device))

            if number <= 16:
                for k in range(number):
                    act(k)
            else:
                pl.loop(0, number)(act)

    def count_all(numbers):
        for number, which, is_near in kinds:

            def add(k, numbers, which=which, is_near=is_near):
                valid, device = which(k)
                above = place(*device) > mine
                no = jnp.logical_not(one)
                if is_near is None:
                    found = (
                        jnp.logical_not(above), no, no,
                        above if which is to_targets else no, above if which is to_facing else no,
                    )
                else:
                    close = is_near(device[1])
                    found = (
                        jnp.logical_not(above),
                        jnp.logical_and(above, close),
                        jnp.logical_and(above, jnp.logical_not(close)),
                        no,
                        no,
                    )
                return tuple(n + jnp.where(jnp.logical_and(valid, f), 1, 0) for n, f in zip(numbers, found))

            if number <= 16:
                for k in range(number):
                    numbers = add(k, numbers)
            else:
                numbers = lax.fori_loop(0, number, add, numbers)
        return numbers

    greet(barrier, (r + 1 - 2 * parity, c))
    greet_all(False)
    zero = jnp.int32(0)
    n_below, n_near_above, n_far_above, n_region_above, n_facing_above = count_all((jnp.int32(1), zero, zero, zero, zero))

    for load in loads[3:]:
        load.start()
    pl.semaphore_wait(barrier, n_below)
    greet_all(True)
    for load in loads[:3]:
        load.wait()
    leaf_low = dot(basis_col[...], table[0], ((1,), (1,))).astype(BF16)
    leaf_send[...] = leaf_low
    up = dot(transfer_col[...], leaf_low, ((0,), (0,))).astype(BF16)
    for j in range(n_red):
        up_send[j] = up[j * chunk : (j + 1) * chunk]

    def remote(src, dst, send_sem, recv_sem, target):
        return pltpu.make_async_remote_copy(
            src_ref=src, dst_ref=dst, send_sem=send_sem, recv_sem=recv_sem,
            device_id=target, device_id_type=MESH,
        )

    side = lax.rem(c, 2)
    passes, direct = side == 0, side == 1
    partner = (r + 1 - 2 * parity, c)
    odd, even = parity == 1, parity == 0
    group = -(-band // own_sems.shape[0])
    spans = [(j, min(group, band - j)) for j in range(0, band, group)]

    pieces = near_recv_sems.shape[1]
    part = table.shape[1] // pieces

    def near_copies(source, cell, target):
        return [
            remote(
                table.at[source, pl.ds(p * part, part)], table.at[cell, pl.ds(p * part, part)],
                group_sems.at[2],
                group_sems.at[5 + cell] if REACH <= cell < 2 * REACH else near_recv_sems.at[cell - 1 - (REACH if cell > 2 else 0), p],
                target,
            )
            for p in range(pieces)
        ]

    beside = (r, c + 1 - 2 * side)
    near = {
        2 * REACH: near_copies(0, 2 * REACH, behind(2, 0)),
        2: near_copies(0, 2, behind(0, 2)),
        2 * REACH + 2: near_copies(2 * REACH, 2 * REACH + 2, behind(0, 2)),
    }
    last, end = c >= cols - near_reach, c == cols - 1
    around = {e: near_copies(e, 2 * REACH + e, behind(2, 0)) for e in (1, 2)}
    first_to_end = near_copies(0, 1, (r, cols - 1))
    for d in (0, 2):
        near[d * REACH + 1] = near_copies(d * REACH + 2 * (1 - side), d * REACH + 1, beside)
    for e in range(REACH):
        near[REACH + e] = near_copies(2 * REACH * (1 - parity) + e, REACH + e, partner)

    chunks = [
        remote(
            up_send.at[j],
            chunk_buf.at[lax.rem(c + cols - (first_red + j), cols)],
            group_sems.at[0],
            group_sems.at[1],
            (r, first_red + j),
        )
        for j in range(n_red)
    ]
    leaves = [
        remote(leaf_send, leaf_buf.at[j], group_sems.at[7], own_sems.at[j // group], behind(0, REACH + j))
        for j in range(band)
    ]
    band_up = [
        remote(
            leaf_buf.at[pl.ds(j, n)], leaf_buf.at[pl.ds(2 * band + j, n)],
            group_sems.at[3], up_recv_sems.at[j // group], behind(2, 0),
        )
        for j, n in spans
    ]
    band_across = [
        remote(
            leaf_buf.at[pl.ds(2 * band * (1 - parity) + j, n)], leaf_buf.at[pl.ds(band + j, n)],
            group_sems.at[3], group_sems.at[6], partner,
        )
        for j, n in spans
    ]

    def known(target, stage, is_near=None):
        below = place(*target) < mine
        if stage == 0:
            return below
        close = near_column(target[1])
        return jnp.logical_and(jnp.logical_not(below), close if stage == 1 else jnp.logical_not(close))

    def start_all(copies, condition):
        for copy in copies:
            when(condition, copy.start)

    def sends(stage):
        for j in range(n_red):
            target = (r, first_red + j)
            when(jnp.logical_and(known(target, stage), target[1] != c), chunks[j].start)
        for j in range(band):
            when(known(behind(0, REACH + j), stage), leaves[j].start)
        if stage != 2:
            start_all(near[2], known(behind(0, 2), stage))
        if stage == 0:
            start_all(near[1], direct)
        if stage == 0:
            start_all(near[2 * REACH], known(behind(2, 0), stage))

    sends(0)
    when(n_facing_above > 0, lambda: pl.semaphore_wait(facing_sem, n_facing_above))
    start_all(near[2 * REACH], jnp.logical_not(known(behind(2, 0), 0)))
    when(n_near_above > 0, lambda: pl.semaphore_wait(near_sem, n_near_above))
    sends(1)

    for near_copy in near[REACH]:
        when(odd, near_copy.start)
    for load in loads[3:]:
        load.wait()

    count = count_ref[0, 0]

    sources = [source_ref[s] for s in range(source_ref.shape[0])]
    slots = []
    for cell in range(len(sources)):
        slot = jnp.int32(0)
        for s, source in enumerate(sources):
            slot = jnp.where(source == cell, s, slot)
        slots.append(slot)

    def term(cell):
        slot = slots[cell]
        source = table[cell]
        source = jnp.where(slot < count, source, jnp.zeros_like(source))
        return dot(source, blocks[slot], ((1,), (0,)))

    total = term(0)
    wraps = known(behind(0, 2), 2)

    def facing_arrived(pass_on):
        for p in range(pieces):
            near[2 * REACH][p].wait_recv()
            if pass_on:
                near[2 * REACH + 2][p].start()
            when(direct, near[2 * REACH + 1][p].start)
            when(even, near[REACH][p].start)

    when(wraps, lambda: facing_arrived(False))
    when(n_far_above > 0, lambda: pl.semaphore_wait(far_sem, n_far_above))
    sends(2)

    follows = jnp.logical_and(c >= near_reach, c < 2 * near_reach)
    own_band = leaf_buf.at[pl.ds(0, band)]

    def leaves_sent():
        pltpu.make_async_copy(own_band, own_band, group_sems.at[7]).wait()

    def release():
        leaves_sent()
        greet(go_sem, (r, lax.rem(c + cols - near_reach, cols)))

    when(follows, release)

    def wrap():
        pl.semaphore_wait(go_sem, 1)
        start_all(near[2], one)
        start_all(first_to_end, c == 0)

    when(c == 1, wrap)
    arrived = chunk_buf.at[pl.ds(1, cols - 1)]

    def reduce_chunks():
        pltpu.make_async_copy(arrived, arrived, group_sems.at[1]).wait()
        when(n_region_above > 0, lambda: pl.semaphore_wait(region_sem, n_region_above))
        reduced = up_send[jnp.clip(c - first_red, 0, n_red - 1)].astype(F32)
        for e in range(1, cols):
            reduced = reduced + chunk_buf[e].astype(F32)
        reduced_send[...] = reduced.astype(BF16)
        for d in range(REACH, rows):
            for e in range(cols):
                remote(
                    reduced_send, region_buf.at[d - REACH, c - first_red], group_sems.at[4], group_sems.at[5],
                    behind(d, e),
                ).start()

    def got(d, e):
        cell = d * REACH + e
        for p in range(pieces):
            near[cell][p].wait_recv()
            when(odd if d == 0 else even, near[REACH + e][p].start)
            if d == 0:
                when(last if e == 2 else end, around[e][p].start)
            if e == 2:
                on = jnp.logical_and(passes, c != cols - 2)
                when(jnp.logical_and(on, odd) if d == 0 else on, near[cell - 1][p].start)
        if (d, e) == (2, 2):
            start_all(near[1], jnp.logical_and(on, even))

    when(is_red, reduce_chunks)
    when(jnp.logical_not(wraps), lambda: facing_arrived(True))

    def own_groups(lo, hi):
        for g in range(lo, hi):
            j, n = spans[g]
            view = leaf_buf.at[pl.ds(j, n)]
            pltpu.make_async_copy(view, view, own_sems.at[g]).wait()
            band_up[g].start()
            when(odd, band_across[g].start)

    def here(cell):
        view = table.at[cell]
        pltpu.make_async_copy(view, view, group_sems.at[5 + cell]).wait()
        return term(cell)

    def up_groups():
        for g in range(len(spans)):
            band_up[g].wait_recv()
            when(even, band_across[g].start)

    own_groups(0, 1)
    when(c == 0, wrap)
    own_groups(1, len(spans))
    got(0, 2)
    when(end, lambda: got(0, 1))

    def from_beside():
        got(0, 1)
        got(2, 1)

    when(jnp.logical_not(last), lambda: got(2, 2))
    when(passes, from_beside)
    for cell in (2 * REACH, 2):
        total = total + term(cell)
    up_groups()
    when(last, lambda: got(2, 2))
    total = total + term(2 * REACH + 2)
    total = total + here(REACH)
    inner = jnp.logical_and(direct, jnp.logical_not(end))
    when(jnp.logical_and(inner, odd), lambda: got(0, 1))

    pltpu.make_async_copy(region_buf, region_buf, group_sems.at[5]).wait()
    rank, vecs = leaf_buf.shape[1:]
    region_out = None
    for d in range(REACH, rows):
        target = lax.rem(r + d, rows)
        slot = jnp.int32(0)
        for f in range(rows):
            slot = jnp.where(list_ref[f] == target, f, slot)
        region = region_buf[d - REACH].astype(F32).reshape(rank, vecs).astype(BF16)
        product = dot(coupling[slot], region, ((0,), (0,)))
        region_out = product if region_out is None else region_out + product
    leaf_out = dot(transfer_row[...], region_out.astype(BF16), ((0,), (0,)))
    mid_band = leaf_buf.at[pl.ds(band, band)]
    pltpu.make_async_copy(mid_band, mid_band, group_sems.at[6]).wait()
    leaf_out = leaf_out + dot(
        couple[...].reshape(REACH * band * rank, rank),
        leaf_buf[...].reshape(REACH * band * rank, vecs),
        ((0,), (0,)),
    )
    total = total + dot(leaf_out.astype(BF16), basis_row[...], ((0,), (0,)))
    when(direct, lambda: got(2, 1))
    total = total + term(2 * REACH + 1)
    total = total + here(REACH + 2)
    when(jnp.logical_and(inner, even), lambda: got(0, 1))
    total = total + term(1)
    total = total + here(REACH + 1)
    out_ref[...] = total.astype(out_ref.dtype)

    def sent(cells):
        view = table.at[pl.ds(0, cells)]
        pltpu.make_async_copy(view, view, group_sems.at[2]).wait()

    n_sent = table.shape[0] - 1
    short = jnp.logical_or(c == near_reach - 1, c == cols - near_reach)
    when(short, lambda: sent(n_sent - 1))
    when(end, lambda: [sent(n_sent + 1), sent(1)])
    when(jnp.logical_not(jnp.logical_or(short, end)), lambda: sent(n_sent))
    upper_bands = leaf_buf.at[pl.ds(band, 2 * band)]
    pltpu.make_async_copy(upper_bands, upper_bands, group_sems.at[3]).wait()
    when(jnp.logical_not(follows), leaves_sent)

    @pl.when(is_red)
    def _():
        others = up_send.at[pl.ds(1, n_red - 1)]
        pltpu.make_async_copy(others, others, group_sems.at[0]).wait()
        for d in range(REACH, rows):
            pltpu.make_async_copy(chunk_buf, chunk_buf, group_sems.at[4]).wait()

    @pl.when(jnp.logical_not(is_red))
    def _():
        pltpu.make_async_copy(up_send, up_send, group_sems.at[0]).wait()


def per_device(
    vectors,
    near_blocks,
    near_source,
    near_count,
    basis_col,
    transfer_col,
    leaf_couple,
    coupling,
    distant_region_list,
    transfer_row,
    basis_row,
):
    rows, cols = lax.axis_size("row"), lax.axis_size("col")
    vecs, leaf = vectors.shape[2:]
    rank = basis_col.shape[2]
    cells = near_blocks.shape[2]
    band = leaf_couple.shape[3]
    n_red = cols // 4
    groups = min(band, 5)
    groups = -(-band // -(-band // groups))
    hbm = pl.BlockSpec(memory_space=pl.ANY)
    out = pl.pallas_call(
        functools.partial(kernel, rows, cols),
        out_shape=pltpu.VMEM((vecs, leaf), BF16),
        in_specs=[hbm] * 11,
        out_specs=pl.BlockSpec(memory_space=pltpu.VMEM),
        scratch_shapes=[
            pltpu.SMEM((cells,), jnp.int32),
            pltpu.SMEM((1, 1), jnp.int32),
            pltpu.SMEM((rows,), jnp.int32),
            pltpu.VMEM((cells, vecs, leaf), BF16),
            pltpu.VMEM((cells, leaf, leaf), BF16),
            pltpu.VMEM((rank, leaf), BF16),
            pltpu.VMEM((rank, rank), BF16),
            pltpu.VMEM((REACH * band, rank, rank), BF16),
            pltpu.VMEM((rows, rank, rank), BF16),
            pltpu.VMEM((rank, rank), BF16),
            pltpu.VMEM((rank, leaf), BF16),
            pltpu.VMEM((rank, vecs), BF16),
            pltpu.VMEM((n_red, rank // n_red, vecs), BF16),
            pltpu.VMEM((rank // n_red, vecs), BF16),
            pltpu.VMEM((REACH * band, rank, vecs), BF16),
            pltpu.VMEM((cols, rank // n_red, vecs), BF16),
            pltpu.VMEM((rows - REACH, n_red, rank // n_red, vecs), BF16),
            pltpu.SemaphoreType.DMA((4,)),
            pltpu.SemaphoreType.DMA((cells - 1 - REACH, PIECES)),
            pltpu.SemaphoreType.DMA((groups,)),
            pltpu.SemaphoreType.DMA((groups,)),
            pltpu.SemaphoreType.DMA((8 + REACH,)),
            pltpu.SemaphoreType.REGULAR,
            pltpu.SemaphoreType.REGULAR,
            pltpu.SemaphoreType.REGULAR,
            pltpu.SemaphoreType.REGULAR,
            pltpu.SemaphoreType.REGULAR,
        ],
        compiler_params=pltpu.CompilerParams(collective_id=0, has_side_effects=True),
    )(
        near_source[0, 0],
        near_count,
        distant_region_list[0],
        vectors[0, 0],
        near_blocks[0, 0],
        basis_col[0, 0],
        transfer_col[0, 0],
        leaf_couple[0, 0].reshape(REACH * band, rank, rank),
        coupling[0],
        transfer_row[0, 0],
        basis_row[0, 0],
    )
    return out[None, None]


def solution(mesh):
    placed = (
        P("row", "col", None, None),
        P("row", "col", None, None, None),
        P("row", "col", None),
        P("row", "col"),
        P("row", "col", None, None),
        P("row", "col", None, None),
        P("row", "col", None, None, None, None),
        P("row", None, None, None),
        P("row", None),
        P("row", "col", None, None),
        P("row", "col", None, None),
    )
    return jax.shard_map(
        per_device,
        mesh=mesh,
        in_specs=placed,
        out_specs=P("row", "col", None, None),
        check_vma=False,
    )
```
